256 devices in a mesh: row: 32 (over y, x, core), col: 8 (over z).
Axes of the slice: x: 4, y: 4, z: 8, core: 2. Of those that a mesh axis runs over, the one named last changes fastest.
Arguments:
- integrals: bfloat16 [1280, 32, 8192], P('row', None, 'col'), may hold values from -6 to 6
- coeffs: bfloat16 [40960, 4096], P('row', 'col'), may hold values from -0.0546875 to 0.0546875
- mask: int32 [1280, 8], replicated, may hold values from 0 to 1, as said below
- offsets: int32 [1281], replicated, may hold values from 0 to 30720, as said below
- atom_of_slot: int32 [1280], replicated, may hold values from 0 to 1279, as said below
Outputs:
- half_transformed: bfloat16 [4096, 8192], P('row', 'col')
The draws below stay inside these ranges and needn't reach their ends.
Inputs may be any that keep to these rules, and one draw needn't show every extreme that they name: `mask`: 1 marks a significant pair of an atom and a block of 64 window functions. offsets[0] = 0 and offsets[a + 1] - offsets[a] is atom a's number of basis functions, 16 to 32; atoms 2k and 2k + 1 together have 3 * 16; rows of an atom's padded block past its number are padding. `atom_of_slot`: a permutation of the atoms; slot k is held by atom owner k // 40 along row, and atom a's AO-row owner is a // 40; one atom owner holds at least one and at most 2 atoms of any one AO-row owner, and exactly 2 for some pairs.
All inputs are finite; a program needn't handle non-finite values.
Results may differ from the reference program's by a relative error of at most 0.015.
Values may be sent and summed in bfloat16 or wider, within the bound.
A program may use at most 256 MiB of HBM per device.

```python
import jax
import jax.numpy as jnp
from jax import lax

AW = 32
ATOMS_DEV = 40
NOCC = 4096
NAUX = 16
NU_DEV = 64
NATOM = 1280
NBAS = 40960
NU = 512
NVB = 8
CAP = 2
N_ROW = 32


def draw_mask(key, part):
    first_key = jax.random.fold_in(key, 11)
    second_key = jax.random.fold_in(key, 12)
    percent = jax.random.randint(first_key, (N_ROW,), 10, 96)
    rolled = jax.random.randint(second_key, (NATOM, NVB), 0, 100)
    owner = jnp.arange(NATOM, dtype=jnp.int32) // ATOMS_DEV
    return (rolled < percent[owner][:, None]).astype(jnp.int32)


def draw_offsets(key, part):
    firsts = jax.random.randint(jax.random.fold_in(key, 21), (NATOM // 2,), AW // 2, AW + 1)
    seconds = 3 * AW // 2 - firsts
    counts = jnp.stack([firsts, seconds], axis=1).reshape(-1).astype(jnp.int32)
    return jnp.concatenate([jnp.zeros((1,), jnp.int32), jnp.cumsum(counts).astype(jnp.int32)])


def draw_atom_of_slot(key, part):
    first_key = jax.random.fold_in(key, 31)
    second_key = jax.random.fold_in(key, 32)
    third_key = jax.random.fold_in(key, 33)
    fourth_key = jax.random.fold_in(key, 34)
    every_shift = jax.random.permutation(first_key, jnp.arange(N_ROW, dtype=jnp.int32))
    repeated = jnp.tile(jnp.arange(N_ROW, dtype=jnp.int32), CAP - 1)
    extra = jax.random.permutation(third_key, repeated)[:ATOMS_DEV - N_ROW]
    shifts = jax.random.permutation(fourth_key, jnp.concatenate([every_shift, extra]).astype(jnp.int32))
    locals_table = jax.vmap(lambda owner: jax.random.permutation(jax.random.fold_in(second_key, owner), ATOMS_DEV))(jnp.arange(N_ROW, dtype=jnp.int32))
    source = jnp.arange(N_ROW, dtype=jnp.int32)[:, None]
    layer = jnp.arange(ATOMS_DEV, dtype=jnp.int32)[None, :]
    target = (source - shifts[None, :]) % N_ROW
    chosen = locals_table[target, jnp.broadcast_to(layer, target.shape)].astype(jnp.int32)
    return (target * ATOMS_DEV + chosen).reshape(-1).astype(jnp.int32)


def strengthened(drawn, stream_key, source, target, parts, factor):
    def block_of(axis_at):
        return (jnp.arange(drawn.shape[axis_at]) // (drawn.shape[axis_at] // parts)).reshape((-1,) + (1,) * (drawn.ndim - 1 - axis_at))

    one_side = jax.random.permutation(stream_key, parts)[block_of(target)]
    second = (block_of(target) + parts // 2) % parts
    return jnp.where((block_of(source) == one_side) | (block_of(source) == second), factor * drawn, drawn)


def block_levels(rng, dims, split, smallest, largest):
    level = 1.0
    for position, shards_of in split:
        steps = jax.random.uniform(jax.random.fold_in(jax.random.fold_in(rng, 6), position), (shards_of,), jnp.float32, smallest / len(split), largest / len(split))
        level = level * jnp.repeat(jnp.exp(steps), dims[position] // shards_of).reshape((-1,) + (1,) * (len(dims) - 1 - position))
    return level


def normal_values(own_key, extent, spread, bound, shards=(), kind=jnp.bfloat16):
    result = spread * jax.random.normal(own_key, extent, jnp.float32)
    if shards:
        result = result * block_levels(own_key, extent, shards, -0.22, 0.18)
    return jnp.clip(result, -bound, bound).astype(kind)


def gaussian_with(rng, dims, scale, reach, cuts, heavy, held_as=jnp.bfloat16):
    drawn = scale * jax.random.normal(rng, dims, jnp.float32)
    if cuts:
        drawn = drawn * block_levels(rng, dims, cuts, -0.22, 0.18)
    return jnp.clip(strengthened(drawn, jax.random.fold_in(rng, 3), *heavy), -reach, reach).astype(held_as)


def setup_inputs(seed: int = 0) -> dict:
    key_list = jax.random.split(jax.random.key(seed), 6)
    return {
        "integrals": normal_values(key_list[0], (NATOM, AW, NU * NAUX), 1.0, 6.0, ((0, 32), (2, 8))),
        "coeffs": gaussian_with(key_list[1], (NBAS, NOCC), NBAS ** -0.5, 0.0546875, ((0, 32), (1, 8)), (0, 1, 32, 2.75)),
        "mask": draw_mask(jax.random.fold_in(key_list[5], 71), 0),
        "offsets": draw_offsets(jax.random.fold_in(key_list[5], 71), 0),
        "atom_of_slot": draw_atom_of_slot(jax.random.fold_in(key_list[5], 71), 0),
    }


def reference(integrals, coeffs, mask, offsets, atom_of_slot):
    natoms = integrals.shape[0]
    inverse = jnp.zeros((natoms,), jnp.int32).at[atom_of_slot].set(jnp.arange(natoms, dtype=jnp.int32))
    ordered = integrals[inverse]
    lengths = offsets[1:] - offsets[:-1]
    row_live = (jnp.arange(AW, dtype=jnp.int32)[None, :] < lengths[:, None]).astype(jnp.bfloat16)
    column_live = jnp.repeat(mask, NU_DEV * NAUX, axis=1).astype(jnp.bfloat16)
    kept = ordered * row_live[:, :, None] * column_live[:, None, :]
    width = kept.shape[2]
    kept_groups = kept.reshape(N_ROW, ATOMS_DEV * AW, width)
    coeff_groups = coeffs.reshape(N_ROW, ATOMS_DEV * AW, coeffs.shape[1])

    def add_owner(total, pieces):
        coeff_piece, kept_piece = pieces
        part = lax.dot_general(coeff_piece, kept_piece, (((0,), (0,)), ((), ())), preferred_element_type=jnp.float32)
        part = lax.optimization_barrier(part.astype(jnp.bfloat16))
        return total + part.astype(jnp.float32), None

    start = jnp.zeros((coeffs.shape[1], width), jnp.float32)
    half, unused = lax.scan(add_owner, start, (coeff_groups, kept_groups))
    return half.astype(jnp.bfloat16)
```

```python
import functools

import jax
import jax.numpy as jnp
from jax import lax
from jax.experimental import pallas as pl
from jax.experimental.pallas import tpu as pltpu
from jax.sharding import PartitionSpec as P

MESH = pl.DeviceIdType.MESH
BF = jnp.bfloat16
F32 = jnp.float32

ROUNDS = 8
LAG = 2.0
AHEAD = 2
V_READY = 56.0
SLOT_US = 2.85


def hops(p):
    return (4, 3) if p % 2 == 0 else (3, 4)


def build_schedule():
    events = []
    done = [0.0] * ROUNDS
    for p in range(ROUNDS):
        for side in range(2):
            for h in range(1, hops(p)[side] + 1):
                key = 3.5 * p + LAG * (h - 1)
                if h == 1:
                    key -= 3.5 * AHEAD
                events.append((max(key, 0.0) * SLOT_US + 4.0, 0, p, h, side))
                last = 3.5 * p + LAG * h
                done[p] = max(done[p], last * SLOT_US + 4.0)
    events.append((V_READY, 1, 0, 0, 0))
    clock = V_READY + 3.0
    for p in range(ROUNDS):
        clock = max(clock, done[p])
        events.append((clock, 2, p, 0, 0))
        events.append((clock + 2.5, 3, p, 0, 0))
        events.append((clock + 7.0, 4, p, 0, 0))
        events.append((clock + 10.5, 5, p, 0, 0))
        clock += 1.4
    return sorted(events)


def kernel(
    pack_s, unpack_s, sig_s, off_s, coef_hbm, v_hbm, out_ref,
    vin, cin, vsend, vrecv, ct, smat, gath, vord, vc, psend, own, prec, q, rb1, red, rb2,
    load_sem, a_send, a_recv, g_send, g_recv, d_send, d_recv, s_send, s_recv, t_send, t_recv,
):
    row = lax.axis_index("row")
    z = lax.axis_index("col")
    core = lax.rem(row, 2)
    chip = lax.div(row, 2)
    x = lax.rem(chip, 4)
    y = lax.div(chip, 4)
    zr = lax.rem(z + 1, 8)
    zl = lax.rem(z + 7, 8)

    load_c = pltpu.make_async_copy(coef_hbm, cin, load_sem.at[0])
    load_v = pltpu.make_async_copy(v_hbm, vin, load_sem.at[1])
    load_c.start()
    load_v.start()

    barrier = pltpu.get_barrier_semaphore()

    def greet(k, carry):
        peer = lax.rem(row + k, 32)
        pl.semaphore_signal(barrier, inc=1, device_id=(peer, z), device_id_type=MESH)
        return carry

    lax.fori_loop(1, 32, greet, 0)
    for side in (zr, zl):
        pl.semaphore_signal(barrier, inc=1, device_id=(row, side), device_id_type=MESH)

    m = lax.broadcasted_iota(jnp.int32, (48, 512), 0)
    k = lax.broadcasted_iota(jnp.int32, (48, 512), 1)
    for g in range(20):
        length = off_s[2 * g + 1] - off_s[2 * g]
        src = jnp.where(m < length, m, 32 + m - length) + 64 * (g % 8)
        smat[48 * g:48 * g + 48, :] = jnp.where(k == src, 1.0, 0.0).astype(BF)
    smat[960:1024, :] = jnp.zeros((64, 512), BF)

    load_c.wait()
    rho = lax.broadcasted_iota(jnp.int32, (512, 512), 0)
    col = lax.broadcasted_iota(jnp.int32, (512, 512), 1)
    want = (rho & 15) + 16 * (rho >> 6) + 256 * ((rho >> 4) & 1) + 128 * ((rho >> 5) & 1)
    perm = jnp.where(col == want, 1.0, 0.0).astype(BF)
    for b in range(5):
        ct[:, 256 * b:256 * b + 256] = lax.dot_general(
            perm, cin[256 * b:256 * b + 256, :], (((1,), (1,)), ((), ())), preferred_element_type=F32
        ).astype(BF)
    for b, (k0, kw, c0, cw) in enumerate(((0, 512, 0, 384), (512, 512, 384, 384), (1024, 256, 768, 256))):
        piece = lax.dot_general(
            ct[:, k0:k0 + kw], smat[c0:c0 + cw, 0:kw], (((1,), (1,)), ((), ())), preferred_element_type=F32
        ).astype(BF)
        gath[:, z, :, c0:c0 + cw] = piece.reshape(8, 64, cw)

    pl.semaphore_wait(barrier, 33)

    def ring(p, h, side):
        src = lax.rem(z + (8 - (h - 1)), 8) if side == 0 else lax.rem(z + (h - 1), 8)
        return pltpu.make_async_remote_copy(
            src_ref=gath.at[p, src],
            dst_ref=gath.at[p, src],
            send_sem=g_send.at[side, p, h - 1],
            recv_sem=g_recv.at[side, p, h - 1],
            device_id=(row, zr if side == 0 else zl),
            device_id_type=MESH,
        )

    def ring_arrival(p, h, side):
        src = lax.rem(z + (8 - h), 8) if side == 0 else lax.rem(z + h, 8)
        pltpu.make_async_remote_copy(
            src_ref=gath.at[p, src],
            dst_ref=gath.at[p, src],
            send_sem=g_send.at[side, p, h - 1],
            recv_sem=g_recv.at[side, p, h - 1],
            device_id=(row, zr if side == 0 else zl),
            device_id_type=MESH,
        ).wait_recv()

    def exchange(k):
        peer = lax.rem(row + k, 32)
        return pltpu.make_async_remote_copy(
            src_ref=vsend.at[pl.ds(2 * peer, 2)],
            dst_ref=vrecv.at[pl.ds(2 * row, 2)],
            send_sem=a_send.at[peer],
            recv_sem=a_recv.at[row],
            device_id=(peer, z),
            device_id_type=MESH,
        )

    def exchange_arrival(k):
        peer = lax.rem(row + k, 32)
        pltpu.make_async_remote_copy(
            src_ref=vsend.at[pl.ds(2 * peer, 2)],
            dst_ref=vrecv.at[pl.ds(2 * peer, 2)],
            send_sem=a_send.at[peer],
            recv_sem=a_recv.at[peer],
            device_id=(peer, z),
            device_id_type=MESH,
        ).wait_recv()

    def pack_and_send():
        load_v.wait()

        def step(k, carry):
            peer = lax.rem(row + k, 32)
            for s in range(2):
                vsend[2 * peer + s] = vin[pack_s[2 * peer + s]]
            exchange(k).start()
            return carry

        lax.fori_loop(1, 32, step, 0)
        for s in range(2):
            vrecv[2 * row + s] = vin[pack_s[2 * row + s]]

    def receive_blocks():
        def wait_one(k, carry):
            exchange_arrival(k)
            return carry

        lax.fori_loop(1, 32, wait_one, 0)

        def place(a, carry):
            live = jnp.full((32, 1024), sig_s[a], jnp.int32).astype(F32).astype(BF)
            vord[pl.ds(pl.multiple_of(32 * a, 32), 32), :] = vrecv[unpack_s[a]] * live
            return carry

        lax.fori_loop(0, 40, place, 0)
        for k0, kw, c0, cw in ((0, 512, 0, 384), (512, 512, 384, 384), (1024, 256, 768, 256)):
            for n in range(4):
                vc[c0:c0 + cw, 256 * n:256 * n + 256] = jnp.dot(
                    smat[c0:c0 + cw, 0:kw], vord[k0:k0 + kw, 256 * n:256 * n + 256], preferred_element_type=F32
                ).astype(BF)

    partner = row + 1 - 2 * core

    def pair_copy(p):
        return pltpu.make_async_remote_copy(
            src_ref=psend.at[p],
            dst_ref=prec.at[p],
            send_sem=d_send.at[p],
            recv_sem=d_recv.at[p],
            device_id=(partner, z),
            device_id_type=MESH,
        )

    def multiply(p):
        theirs = pl.multiple_of(32 * (1 - core), 32)
        mine = pl.multiple_of(32 * core, 32)
        lhs = gath[p, :, pl.ds(theirs, 32), :].reshape(256, 1024)

        for n in range(4):
            psend[p, :, 256 * n:256 * n + 256] = jnp.dot(
                lhs, vc[:, 256 * n:256 * n + 256], preferred_element_type=F32
            ).astype(BF)
        pair_copy(p).start()
        lhs2 = gath[p, :, pl.ds(mine, 32), :].reshape(256, 1024)
        for n in range(4):
            own[p, :, 256 * n:256 * n + 256] = jnp.dot(
                lhs2, vc[:, 256 * n:256 * n + 256], preferred_element_type=F32
            )

    def row_of(yy, xx):
        return (yy * 4 + xx) * 2 + core

    def first_copy(p, half, d):
        if half == 0:
            to = lax.rem(y + d, 4)
            src, dev = q.at[p, to, :, :, 0:512], row_of(to, x)
        else:
            to = lax.rem(x + d, 4)
            src, dev = q.at[p, :, to, :, 512:1024], row_of(y, to)
        return pltpu.make_async_remote_copy(
            src_ref=src,
            dst_ref=rb1.at[p, half, d - 1],
            send_sem=s_send.at[p, half, d - 1],
            recv_sem=s_recv.at[p, half, d - 1],
            device_id=(dev, z),
            device_id_type=MESH,
        )

    def second_copy(p, half, d):
        if half == 0:
            to = lax.rem(x + d, 4)
            dev = row_of(y, to)
        else:
            to = lax.rem(y + d, 4)
            dev = row_of(to, x)
        return pltpu.make_async_remote_copy(
            src_ref=red.at[p, half, to],
            dst_ref=rb2.at[p, half, d - 1],
            send_sem=t_send.at[p, half, d - 1],
            recv_sem=t_recv.at[p, half, d - 1],
            device_id=(dev, z),
            device_id_type=MESH,
        )

    def pair_sum(p):
        pair_copy(p).wait_recv()
        q[p] = (own[p] + prec[p].astype(F32)).astype(BF).reshape(4, 4, 16, 1024)
        for d in (2, 1, 3):
            for half in range(2):
                first_copy(p, half, d).start()

    def first_sum(p):
        for d in (1, 3, 2):
            for half in range(2):
                first_copy(p, half, d).wait_recv()
        for half in range(2):
            mine = q[p, y, :, :, 0:512] if half == 0 else q[p, :, x, :, 512:1024]
            total = mine.astype(F32)
            for d in range(3):
                total = total + rb1[p, half, d].astype(F32)
            red[p, half] = total.astype(BF)
        for d in (2, 1, 3):
            for half in range(2):
                second_copy(p, half, d).start()

    def second_sum(p):
        for d in (1, 3, 2):
            for half in range(2):
                second_copy(p, half, d).wait_recv()
        for half in range(2):
            total = red[p, half, x if half == 0 else y].astype(F32)
            for d in range(3):
                total = total + rb2[p, half, d].astype(F32)
            out_ref[16 * p:16 * p + 16, 512 * half:512 * half + 512] = total.astype(BF)

    packed = False
    for when, kind, p, h, side in build_schedule():
        if kind == 0:
            if h > 1:
                if not packed:
                    pack_and_send()
                    packed = True
                ring_arrival(p, h - 1, side)
            ring(p, h, side).start()
        elif kind == 1:
            receive_blocks()
        elif kind == 2:
            for s in range(2):
                ring_arrival(p, hops(p)[s], s)
            multiply(p)
        elif kind == 3:
            pair_sum(p)
        elif kind == 4:
            first_sum(p)
        else:
            second_sum(p)

    def sent(k, carry):
        exchange(k).wait_send()
        return carry

    lax.fori_loop(1, 32, sent, 0)
    for p in range(ROUNDS):
        for side in range(2):
            for h in range(1, hops(p)[side] + 1):
                ring(p, h, side).wait_send()
        pair_copy(p).wait_send()
        for d in (1, 2, 3):
            for half in range(2):
                first_copy(p, half, d).wait_send()
                second_copy(p, half, d).wait_send()


def body(integrals, coeffs, mask, offsets, atom_of_slot):
    me = lax.axis_index("row")
    col = lax.axis_index("col")
    holders = atom_of_slot.reshape(32, 40)
    counter = jnp.arange(40, dtype=jnp.int32)
    target = lax.dynamic_slice_in_dim(atom_of_slot, me * 40, 40) // 40
    rank = jnp.sum(((target[None, :] == target[:, None]) & (counter[None, :] < counter[:, None])).astype(jnp.int32), axis=1)
    slot = jnp.arange(64, dtype=jnp.int32)
    pack = jnp.sum(jnp.where((2 * target + rank)[None, :] == slot[:, None], counter[None, :], 0), axis=1)
    mine = holders // 40 == me
    arrival = jnp.cumsum(mine.astype(jnp.int32), axis=1) - 1
    place = 2 * jnp.arange(32, dtype=jnp.int32)[:, None] + arrival
    local = jnp.where(mine, holders - me * 40, -1)
    unpack = jnp.sum(jnp.where(local[None] == counter[:, None, None], place[None], 0), axis=(1, 2))
    sig = (lax.dynamic_slice(mask, (me * 40, col), (40, 1))[:, 0] > 0).astype(jnp.int32)
    off = lax.dynamic_slice_in_dim(offsets, me * 40, 41)

    smem = pl.BlockSpec(memory_space=pltpu.SMEM)
    hbm = pl.BlockSpec(memory_space=pl.ANY)
    vmem = pltpu.VMEM
    dma = pltpu.SemaphoreType.DMA
    return pl.pallas_call(
        kernel,
        out_shape=jax.ShapeDtypeStruct((128, 1024), BF),
        in_specs=[smem, smem, smem, smem, hbm, hbm],
        out_specs=pl.BlockSpec(memory_space=pltpu.VMEM),
        scratch_shapes=[
            vmem((40, 32, 1024), BF),
            vmem((1280, 512), BF),
            vmem((64, 32, 1024), BF),
            vmem((64, 32, 1024), BF),
            vmem((512, 1280), BF),
            vmem((1024, 512), BF),
            vmem((ROUNDS, 8, 64, 1024), BF),
            vmem((1280, 1024), BF),
            vmem((1024, 1024), BF),
            vmem((ROUNDS, 256, 1024), BF),
            vmem((ROUNDS, 256, 1024), F32),
            vmem((ROUNDS, 256, 1024), BF),
            vmem((ROUNDS, 4, 4, 16, 1024), BF),
            vmem((ROUNDS, 2, 3, 4, 16, 512), BF),
            vmem((ROUNDS, 2, 4, 16, 512), BF),
            vmem((ROUNDS, 2, 3, 16, 512), BF),
            dma((2,)),
            dma((32,)),
            dma((32,)),
            dma((2, ROUNDS, 4)),
            dma((2, ROUNDS, 4)),
            dma((ROUNDS,)),
            dma((ROUNDS,)),
            dma((ROUNDS, 2, 3)),
            dma((ROUNDS, 2, 3)),
            dma((ROUNDS, 2, 3)),
            dma((ROUNDS, 2, 3)),
        ],
        compiler_params=pltpu.CompilerParams(
            collective_id=0, has_side_effects=True, vmem_limit_bytes=66_000_000
        ),
    )(pack, unpack, sig, off, coeffs, integrals)


def solution(mesh):
    in_specs = (P("row", None, "col"), P("row", "col"), P(), P(), P())
    return jax.shard_map(body, mesh=mesh, in_specs=in_specs, out_specs=P("row", "col"), check_vma=False)
```

```python
import functools

import jax
import jax.numpy as jnp
from jax import lax
from jax.experimental import pallas as pl
from jax.experimental.pallas import tpu as pltpu
from jax.sharding import PartitionSpec as P

MESH = pl.DeviceIdType.MESH
BF = jnp.bfloat16
F32 = jnp.float32

ROUNDS = 8
LAG = 2.0
AHEAD = 2
V_READY = 70.0
SLOT_US = 2.8
START = 4.0
FAR = ((2, 2), (2, 0), (0, 2), (3, 2), (1, 2), (2, 3), (2, 1), (3, 1), (3, 3), (1, 3), (1, 1), (3, 0), (0, 3), (1, 0), (0, 1))


def hops(p):
    return (4, 3) if p % 2 == 0 else (3, 4)


def build_schedule():
    events = []
    done = [0.0] * ROUNDS
    for p in range(ROUNDS):
        for side in range(2):
            for h in range(1, hops(p)[side] + 1):
                key = 3.5 * p + LAG * (h - 1)
                if h == 1:
                    key -= 3.5 * AHEAD
                events.append((max(key, 0.0) * SLOT_US + START, 0, p, h, side))
                last = 3.5 * p + LAG * h
                done[p] = max(done[p], last * SLOT_US + START)
    events.append((V_READY, 1, 0, 0, 0))
    clock = V_READY + 3.0
    for p in range(ROUNDS):
        clock = max(clock, done[p])
        events.append((clock, 2, p, 0, 0))
        events.append((clock + 2.5, 3, p, 0, 0))
        events.append((clock + 7.0, 4, p, 0, 0))
        events.append((clock + 10.5, 5, p, 0, 0))
        clock += 1.4
    return sorted(events)


def kernel(
    off_s, holder_hbm, mask_hbm, coef_hbm, v_hbm, out_ref,
    holder, mask, table, table_s,
    vin, cin, vsend, vrecv, ct, smat, gath, vord, vc, vtail, psend, own, prec, q, rb1, red, rb2,
    load_sem, a_send, a_recv, g_send, g_recv, d_send, d_recv, s_send, s_recv, t_send, t_recv,
):
    row = lax.axis_index("row")
    z = lax.axis_index("col")
    core = lax.rem(row, 2)
    chip = lax.div(row, 2)
    x = lax.rem(chip, 4)
    y = lax.div(chip, 4)
    zr = lax.rem(z + 1, 8)
    zl = lax.rem(z + 7, 8)

    load_c = pltpu.make_async_copy(coef_hbm, cin, load_sem.at[0])
    load_v = pltpu.make_async_copy(v_hbm, vin, load_sem.at[1])
    load_c.start()
    load_h = pltpu.make_async_copy(holder_hbm, holder, load_sem.at[2])
    load_m = pltpu.make_async_copy(mask_hbm, mask, load_sem.at[3])
    load_h.start()
    load_m.start()
    load_v.start()

    barrier = pltpu.get_barrier_semaphore()

    def greet(k, carry):
        peer = lax.rem(row + k, 32)
        pl.semaphore_signal(barrier, inc=1, device_id=(peer, z), device_id_type=MESH)
        return carry

    lax.fori_loop(1, 32, greet, 0)
    for side in (zr, zl):
        pl.semaphore_signal(barrier, inc=1, device_id=(row, side), device_id_type=MESH)

    m = lax.broadcasted_iota(jnp.int32, (48, 512), 0)
    k = lax.broadcasted_iota(jnp.int32, (48, 512), 1)
    for g in range(20):
        at = row * 40 + 2 * g
        length = off_s[at + 1] - off_s[at]
        src = jnp.where(m < length, m, 32 + m - length) + 64 * (g % 8)
        rows = jnp.where(k == src, 1.0, 0.0).astype(BF)
        if g < 18:
            smat[48 * g:48 * g + 48, :] = rows
        elif g == 18:
            smat[864:896, :] = rows[0:32]
            smat[960:976, :] = rows[32:48]
        else:
            smat[976:1024, :] = rows
    smat[896:960, :] = jnp.zeros((64, 512), BF)
    smat[1024:1088, :] = jnp.zeros((64, 512), BF)

    load_c.wait()
    rho = lax.broadcasted_iota(jnp.int32, (512, 512), 0)
    col = lax.broadcasted_iota(jnp.int32, (512, 512), 1)
    want = (rho & 15) + 256 * ((rho >> 4) & 1) + 16 * ((rho >> 5) & 7) + 128 * (rho >> 8)
    perm = jnp.where(col == want, 1.0, 0.0).astype(BF)
    for b in range(5):
        ct[:, 256 * b:256 * b + 256] = lax.dot_general(
            perm, cin[256 * b:256 * b + 256, :], (((1,), (1,)), ((), ())), preferred_element_type=F32
        ).astype(BF)

    def compact(r0, rw, k0, kw, c0, cw):
        return lax.dot_general(
            ct[r0:r0 + rw, k0:k0 + kw], smat[c0:c0 + cw, 0:kw], (((1,), (1,)), ((), ())), preferred_element_type=F32
        )

    for t0, k0, kw, c0, cw in ((0, 0, 512, 0, 384), (3, 512, 512, 384, 384), (6, 1024, 256, 768, 128)):
        piece = compact(0, 512, k0, kw, c0, cw).astype(BF).reshape(2, 8, 32, cw)
        for qc in range(2):
            for t in range(cw // 128):
                gath[:, z, 7 * qc + t0 + t] = piece[qc, :, :, 128 * t:128 * t + 128]
    tail = compact(0, 256, 1024, 256, 960, 128) + compact(256, 256, 1024, 256, 896, 128)
    gath[:, z, 14] = tail.astype(BF).reshape(8, 32, 128)

    pl.semaphore_wait(barrier, 33)

    def ring(p, h, side):
        src = lax.rem(z + (8 - (h - 1)), 8) if side == 0 else lax.rem(z + (h - 1), 8)
        return pltpu.make_async_remote_copy(
            src_ref=gath.at[p, src],
            dst_ref=gath.at[p, src],
            send_sem=g_send.at[side, p, h - 1],
            recv_sem=g_recv.at[side, p, h - 1],
            device_id=(row, zr if side == 0 else zl),
            device_id_type=MESH,
        )

    def ring_arrival(p, h, side):
        src = lax.rem(z + (8 - h), 8) if side == 0 else lax.rem(z + h, 8)
        pltpu.make_async_remote_copy(
            src_ref=gath.at[p, src],
            dst_ref=gath.at[p, src],
            send_sem=g_send.at[side, p, h - 1],
            recv_sem=g_recv.at[side, p, h - 1],
            device_id=(row, zr if side == 0 else zl),
            device_id_type=MESH,
        ).wait_recv()

    def peer_of(k):
        if k == 30:
            return row + 1 - 2 * core
        dy, dx = FAR[k // 2]
        other = core if k % 2 == 0 else 1 - core
        return (lax.rem(y + dy, 4) * 4 + lax.rem(x + dx, 4)) * 2 + other

    def exchange(k):
        peer = peer_of(k)
        return pltpu.make_async_remote_copy(
            src_ref=vsend.at[pl.ds(2 * peer, 2)],
            dst_ref=vrecv.at[pl.ds(2 * row, 2)],
            send_sem=a_send.at[peer],
            recv_sem=a_recv.at[row],
            device_id=(peer, z),
            device_id_type=MESH,
        )

    def exchange_arrival(k):
        peer = lax.rem(row + k, 32)
        pltpu.make_async_remote_copy(
            src_ref=vsend.at[pl.ds(2 * peer, 2)],
            dst_ref=vrecv.at[pl.ds(2 * peer, 2)],
            send_sem=a_send.at[peer],
            recv_sem=a_recv.at[peer],
            device_id=(peer, z),
            device_id_type=MESH,
        ).wait_recv()

    def build_tables():
        load_h.wait()
        load_m.wait()
        lane = lax.broadcasted_iota(jnp.int32, (40, 1280), 1)
        atom = lax.broadcasted_iota(jnp.int32, (40, 1280), 0)
        held = jnp.broadcast_to(holder[...], (40, 1280))
        owner = lax.shift_right_logical(held * 52429, 21)
        slot = jnp.max(jnp.where(held == atom + 40 * row, lane, 0), axis=1, keepdims=True)
        source = lax.shift_right_logical(slot * 52429, 21)
        earlier = (owner == row) & (lane >= 40 * source) & (lane < slot)
        arrive = 2 * source + jnp.max(jnp.where(earlier, 1, 0), axis=1, keepdims=True)
        wanted = jnp.broadcast_to(mask[pl.ds(z, 1), :], (40, 1280))
        live = jnp.sum(jnp.where(lane == atom + 40 * row, wanted, 0), axis=1, keepdims=True)
        place = lane - 40 * row
        here = (owner == atom) & (place >= 0) & (place < 40)
        first = jnp.min(jnp.where(here, place, 39), axis=1, keepdims=True)
        last = jnp.max(jnp.where(here, place, 0), axis=1, keepdims=True)
        diagonal = lax.broadcasted_iota(jnp.int32, (40, 128), 1) == lax.broadcasted_iota(jnp.int32, (40, 128), 0)
        for r, value in enumerate((arrive, live, first, last)):
            table[r:r + 1, :] = jnp.sum(jnp.where(diagonal, value, 0), axis=0, keepdims=True)
        table[4:8, :] = jnp.zeros((4, 128), jnp.int32)
        to_scalar = pltpu.make_async_copy(table, table_s, load_sem.at[4])
        to_scalar.start()
        to_scalar.wait()

    def pack_and_send():
        build_tables()
        load_v.wait()
        for k in range(31):
            peer = peer_of(k)
            for s in range(2):
                vsend[2 * peer + s] = vin[table_s[2 + s, peer]]
            exchange(k).start()
        for s in range(2):
            vrecv[2 * row + s] = vin[table_s[2 + s, row]]

    def receive_blocks():
        def wait_one(k, carry):
            exchange_arrival(k)
            return carry

        lax.fori_loop(1, 32, wait_one, 0)

        def place(a, carry):
            live = jnp.full((32, 1024), table_s[1, a], jnp.int32).astype(F32).astype(BF)
            vord[pl.ds(pl.multiple_of(32 * a, 32), 32), :] = vrecv[table_s[0, a]] * live
            return carry

        lax.fori_loop(0, 40, place, 0)
        for k0, kw, c0, cw in ((0, 512, 0, 384), (512, 512, 384, 384), (1024, 256, 768, 128)):
            for n in range(4):
                vc[c0:c0 + cw, 256 * n:256 * n + 256] = jnp.dot(
                    smat[c0:c0 + cw, 0:kw], vord[k0:k0 + kw, 256 * n:256 * n + 256], preferred_element_type=F32
                ).astype(BF)
        vtail[...] = jnp.dot(smat[896:1088, 0:256], vord[1024:1280, :], preferred_element_type=F32).astype(BF)

    partner = row + 1 - 2 * core

    def pair_copy(p):
        return pltpu.make_async_remote_copy(
            src_ref=psend.at[p],
            dst_ref=prec.at[p],
            send_sem=d_send.at[p],
            recv_sem=d_recv.at[p],
            device_id=(partner, z),
            device_id_type=MESH,
        )

    def product(p, qc, n):
        tiles = [gath[p, :, 7 * qc + t].reshape(256, 128) for t in range(7)] + [gath[p, :, 14].reshape(256, 128)]
        start = pl.multiple_of(64 * (1 - qc), 64)
        rhs = jnp.concatenate(
            [vc[:, 256 * n:256 * n + 256], vtail[pl.ds(start, 128), 256 * n:256 * n + 256]], axis=0
        )
        return jnp.dot(jnp.concatenate(tiles, axis=1), rhs, preferred_element_type=F32)

    def multiply(p):
        for n in range(4):
            psend[p, :, 256 * n:256 * n + 256] = product(p, 1 - core, n).astype(BF)
        pair_copy(p).start()
        for n in range(4):
            own[p, :, 256 * n:256 * n + 256] = product(p, core, n)

    def row_of(yy, xx):
        return (yy * 4 + xx) * 2 + core

    def first_copy(p, half, d):
        if half == 0:
            to = lax.rem(y + d, 4)
            src, dev = q.at[p, to, :, :, 0:512], row_of(to, x)
        else:
            to = lax.rem(x + d, 4)
            src, dev = q.at[p, :, to, :, 512:1024], row_of(y, to)
        return pltpu.make_async_remote_copy(
            src_ref=src,
            dst_ref=rb1.at[p, half, d - 1],
            send_sem=s_send.at[p, half, d - 1],
            recv_sem=s_recv.at[p, half, d - 1],
            device_id=(dev, z),
            device_id_type=MESH,
        )

    def second_copy(p, half, d):
        if half == 0:
            to = lax.rem(x + d, 4)
            dev = row_of(y, to)
        else:
            to = lax.rem(y + d, 4)
            dev = row_of(to, x)
        return pltpu.make_async_remote_copy(
            src_ref=red.at[p, half, to],
            dst_ref=rb2.at[p, half, d - 1],
            send_sem=t_send.at[p, half, d - 1],
            recv_sem=t_recv.at[p, half, d - 1],
            device_id=(dev, z),
            device_id_type=MESH,
        )

    def pair_sum(p):
        pair_copy(p).wait_recv()
        q[p] = (own[p] + prec[p].astype(F32)).astype(BF).reshape(4, 4, 16, 1024)
        for d in (2, 1, 3):
            for half in range(2):
                first_copy(p, half, d).start()

    def first_sum(p):
        for d in (1, 3, 2):
            for half in range(2):
                first_copy(p, half, d).wait_recv()
        for half in range(2):
            mine = q[p, y, :, :, 0:512] if half == 0 else q[p, :, x, :, 512:1024]
            total = mine.astype(F32)
            for d in range(3):
                total = total + rb1[p, half, d].astype(F32)
            red[p, half] = total.astype(BF)
        for d in (2, 1, 3):
            for half in range(2):
                second_copy(p, half, d).start()

    def second_sum(p):
        for d in (1, 3, 2):
            for half in range(2):
                second_copy(p, half, d).wait_recv()
        for half in range(2):
            total = red[p, half, x if half == 0 else y].astype(F32)
            for d in range(3):
                total = total + rb2[p, half, d].astype(F32)
            out_ref[16 * p:16 * p + 16, 512 * half:512 * half + 512] = total.astype(BF)

    packed = False
    for when, kind, p, h, side in build_schedule():
        if kind == 0:
            if h > 1:
                if not packed:
                    pack_and_send()
                    packed = True
                ring_arrival(p, h - 1, side)
            ring(p, h, side).start()
        elif kind == 1:
            receive_blocks()
        elif kind == 2:
            for s in range(2):
                ring_arrival(p, hops(p)[s], s)
            multiply(p)
        elif kind == 3:
            pair_sum(p)
        elif kind == 4:
            first_sum(p)
        else:
            second_sum(p)

    for k in range(31):
        exchange(k).wait_send()
    for p in range(ROUNDS):
        for side in range(2):
            for h in range(1, hops(p)[side] + 1):
                ring(p, h, side).wait_send()
        pair_copy(p).wait_send()
        for d in (1, 2, 3):
            for half in range(2):
                first_copy(p, half, d).wait_send()
                second_copy(p, half, d).wait_send()


def body(integrals, coeffs, mask, offsets, atom_of_slot):
    smem = pl.BlockSpec(memory_space=pltpu.SMEM)
    hbm = pl.BlockSpec(memory_space=pl.ANY)
    vmem = pltpu.VMEM
    dma = pltpu.SemaphoreType.DMA
    return pl.pallas_call(
        kernel,
        out_shape=jax.ShapeDtypeStruct((128, 1024), BF),
        in_specs=[smem, hbm, hbm, hbm, hbm],
        out_specs=pl.BlockSpec(memory_space=pltpu.VMEM),
        scratch_shapes=[
            vmem((1, 1280), jnp.int32),
            vmem((8, 1280), jnp.int32),
            vmem((8, 128), jnp.int32),
            pltpu.SMEM((8, 128), jnp.int32),
            vmem((40, 32, 1024), BF),
            vmem((1280, 512), BF),
            vmem((64, 32, 1024), BF),
            vmem((64, 32, 1024), BF),
            vmem((512, 1280), BF),
            vmem((1088, 512), BF),
            vmem((ROUNDS, 8, 15, 32, 128), BF),
            vmem((1280, 1024), BF),
            vmem((896, 1024), BF),
            vmem((192, 1024), BF),
            vmem((ROUNDS, 256, 1024), BF),
            vmem((ROUNDS, 256, 1024), F32),
            vmem((ROUNDS, 256, 1024), BF),
            vmem((ROUNDS, 4, 4, 16, 1024), BF),
            vmem((ROUNDS, 2, 3, 4, 16, 512), BF),
            vmem((ROUNDS, 2, 4, 16, 512), BF),
            vmem((ROUNDS, 2, 3, 16, 512), BF),
            dma((5,)),
            dma((32,)),
            dma((32,)),
            dma((2, ROUNDS, 4)),
            dma((2, ROUNDS, 4)),
            dma((ROUNDS,)),
            dma((ROUNDS,)),
            dma((ROUNDS, 2, 3)),
            dma((ROUNDS, 2, 3)),
            dma((ROUNDS, 2, 3)),
            dma((ROUNDS, 2, 3)),
        ],
        compiler_params=pltpu.CompilerParams(
            collective_id=0, has_side_effects=True, vmem_limit_bytes=66_000_000
        ),
    )(offsets, atom_of_slot.reshape(1, 1280), mask.T, coeffs, integrals)


def solution(mesh):
    in_specs = (P("row", None, "col"), P("row", "col"), P(), P(), P())
    return jax.shard_map(body, mesh=mesh, in_specs=in_specs, out_specs=P("row", "col"), check_vma=False)
```

```python
import functools

import jax
import jax.numpy as jnp
from jax import lax
from jax.experimental import pallas as pl
from jax.experimental.pallas import tpu as pltpu
from jax.sharding import PartitionSpec as P

MESH = pl.DeviceIdType.MESH
BF = jnp.bfloat16
F32 = jnp.float32

ROUNDS = 8
FAR = ((2, 2), (2, 0), (0, 2), (3, 2), (1, 2), (2, 3), (2, 1), (3, 1), (3, 3), (1, 3), (1, 1), (3, 0), (0, 3), (1, 0), (0, 1))

START = 5.0
SLOT = 2.68
WIRE = 2.4
V_READY = 59.0
LAG = 2


def hops(p):
    return (4, 3) if p % 4 < 2 else (3, 4)


RING_SEM = {
    key: n
    for n, key in enumerate(
        (side, p, h) for p in range(ROUNDS) for side in range(2) for h in range(1, hops(p)[side] + 1)
    )
}


def ring_slots(side):
    slot_of = {}
    slot = 0
    while len(slot_of) < sum(hops(p)[side] for p in range(ROUNDS)):
        for p in range(ROUNDS):
            h = 1
            while (p, h) in slot_of:
                h += 1
            if h <= hops(p)[side] and (h == 1 or slot_of[p, h - 1] + LAG <= slot):
                slot_of[p, h] = slot
                break
        slot += 1
    return slot_of


def build_schedule():
    slots = [ring_slots(side) for side in range(2)]
    landed = lambda p, h, side: START + (slots[side][p, h] + 1) * SLOT + WIRE
    pending = [(V_READY, 1, "blocks", 0, 0, 0)]
    for side in range(2):
        for (p, h), slot in slots[side].items():
            if h == 1:
                pending.append((START + max(0, slot - 2) * SLOT, 0, "ring", p, h, side))
            else:
                pending.append((landed(p, h - 1, side), 0, "ring", p, h, side))
    order, clock, links = [], START, 0.0
    have_blocks = False
    cost = {"ring": 0.02, "blocks": 2.0, "multiply": 1.4, "pair": 0.15, "first": 0.15, "second": 0.05}
    while pending:
        clock = max(clock, min(e[0] for e in pending))
        event = min((e for e in pending if e[0] <= clock), key=lambda e: (e[1], e[3], e[0], e[4]))
        pending.remove(event)
        order.append(event[2:])
        kind, p = event[2:4]
        clock += cost[kind]
        if kind == "blocks":
            for p in range(ROUNDS):
                ready = max(landed(p, hops(p)[side], side) for side in range(2))
                pending.append((ready, 3, "multiply", p, 0, 0))
        elif kind == "multiply":
            pending.append((clock + 1.0, 2, "pair", p, 0, 0))
        elif kind == "pair":
            links = max(links, clock) + 2.75
            pending.append((links + WIRE, 2, "first", p, 0, 0))
        elif kind == "first":
            links = max(links, clock) + 0.7
            pending.append((links + WIRE, 2, "second", p, 0, 0))
    return order


def kernel(
    off_s, holder_hbm, mask_hbm, coef_hbm, v_hbm, out_ref,
    holder, mask, table, table_s,
    vin, cin, vsend, vrecv, ct, smat, gath, vord, vc, vtail, psend, own, prec, q, rb1, red, rb2,
    load_sem, sent, a_recv, g_recv, d_recv, s_recv, t_recv,
):
    row = lax.axis_index("row")
    z = lax.axis_index("col")
    core = lax.rem(row, 2)
    chip = lax.div(row, 2)
    x = lax.rem(chip, 4)
    y = lax.div(chip, 4)
    zr = lax.rem(z + 1, 8)
    zl = lax.rem(z + 7, 8)

    load_c = pltpu.make_async_copy(coef_hbm, cin, load_sem.at[0])
    load_v = pltpu.make_async_copy(v_hbm, vin, load_sem.at[1])
    load_c.start()
    load_h = pltpu.make_async_copy(holder_hbm, holder, load_sem.at[2])
    load_m = pltpu.make_async_copy(mask_hbm, mask, load_sem.at[3])
    load_h.start()
    load_m.start()
    load_v.start()

    barrier = pltpu.get_barrier_semaphore()

    def greet(k, carry):
        peer = lax.rem(row + k, 32)
        pl.semaphore_signal(barrier, inc=1, device_id=(peer, z), device_id_type=MESH)
        return carry

    lax.fori_loop(1, 32, greet, 0)
    for side in (zr, zl):
        pl.semaphore_signal(barrier, inc=1, device_id=(row, side), device_id_type=MESH)

    m = lax.broadcasted_iota(jnp.int32, (48, 512), 0)
    k = lax.broadcasted_iota(jnp.int32, (48, 512), 1)
    for g in range(20):
        at = row * 40 + 2 * g
        length = off_s[at + 1] - off_s[at]
        src = jnp.where(m < length, m, 32 + m - length) + 64 * (g % 8)
        rows = jnp.where(k == src, 1.0, 0.0).astype(BF)
        if g < 18:
            smat[48 * g:48 * g + 48, :] = rows
        elif g == 18:
            smat[864:896, :] = rows[0:32]
            smat[960:976, :] = rows[32:48]
        else:
            smat[976:1024, :] = rows
    smat[896:960, :] = jnp.zeros((64, 512), BF)
    smat[1024:1088, :] = jnp.zeros((64, 512), BF)

    load_c.wait()
    rho = lax.broadcasted_iota(jnp.int32, (512, 512), 0)
    col = lax.broadcasted_iota(jnp.int32, (512, 512), 1)
    want = (rho & 15) + 256 * ((rho >> 4) & 1) + 16 * ((rho >> 5) & 7) + 128 * (rho >> 8)
    perm = jnp.where(col == want, 1.0, 0.0).astype(BF)
    for b in range(5):
        ct[:, 256 * b:256 * b + 256] = lax.dot_general(
            perm, cin[256 * b:256 * b + 256, :], (((1,), (1,)), ((), ())), preferred_element_type=F32
        ).astype(BF)

    def compact(r0, rw, k0, kw, c0, cw):
        return lax.dot_general(
            ct[r0:r0 + rw, k0:k0 + kw], smat[c0:c0 + cw, 0:kw], (((1,), (1,)), ((), ())), preferred_element_type=F32
        )

    for t0, k0, kw, c0, cw in ((0, 0, 512, 0, 384), (3, 512, 512, 384, 384), (6, 1024, 256, 768, 128)):
        piece = compact(0, 512, k0, kw, c0, cw).astype(BF).reshape(2, 8, 32, cw)
        for qc in range(2):
            for t in range(cw // 128):
                gath[:, z, 7 * qc + t0 + t] = piece[qc, :, :, 128 * t:128 * t + 128]
    tail = compact(0, 256, 1024, 256, 960, 128) + compact(256, 256, 1024, 256, 896, 128)
    gath[:, z, 14] = tail.astype(BF).reshape(8, 32, 128)

    pl.semaphore_wait(barrier, 33)

    def ring(p, h, side):
        src = lax.rem(z + (8 - (h - 1)), 8) if side == 0 else lax.rem(z + (h - 1), 8)
        return pltpu.make_async_remote_copy(
            src_ref=gath.at[p, src],
            dst_ref=gath.at[p, src],
            send_sem=sent.at[1],
            recv_sem=g_recv.at[RING_SEM[side, p, h]],
            device_id=(row, zr if side == 0 else zl),
            device_id_type=MESH,
        )

    def ring_arrival(p, h, side):
        src = lax.rem(z + (8 - h), 8) if side == 0 else lax.rem(z + h, 8)
        pltpu.make_async_remote_copy(
            src_ref=gath.at[p, src],
            dst_ref=gath.at[p, src],
            send_sem=sent.at[1],
            recv_sem=g_recv.at[RING_SEM[side, p, h]],
            device_id=(row, zr if side == 0 else zl),
            device_id_type=MESH,
        ).wait_recv()

    def place_of(k):
        if k == 30:
            return row + 1 - 2 * core
        dy, dx = FAR[k // 2]
        other = core if k % 2 == 0 else 1 - core
        return (lax.rem(y + dy, 4) * 4 + lax.rem(x + dx, 4)) * 2 + other

    def peer_of(k):
        return jnp.where(core == 0, place_of(k), place_of(30 - k))

    def exchange(k):
        peer = peer_of(k)
        return pltpu.make_async_remote_copy(
            src_ref=vsend.at[pl.ds(2 * peer, 2)],
            dst_ref=vrecv.at[pl.ds(2 * row, 2)],
            send_sem=sent.at[0],
            recv_sem=a_recv.at[0],
            device_id=(peer, z),
            device_id_type=MESH,
        )

    def all_of(ref, send_sem, recv_sem):
        return pltpu.make_async_remote_copy(
            src_ref=ref, dst_ref=ref, send_sem=send_sem, recv_sem=recv_sem,
            device_id=(row, zr), device_id_type=MESH,
        )

    def build_tables():
        load_h.wait()
        load_m.wait()
        lane = lax.broadcasted_iota(jnp.int32, (40, 1280), 1)
        atom = lax.broadcasted_iota(jnp.int32, (40, 1280), 0)
        held = jnp.broadcast_to(holder[...], (40, 1280))
        owner = lax.shift_right_logical(held * 52429, 21)
        slot = jnp.max(jnp.where(held == atom + 40 * row, lane, 0), axis=1, keepdims=True)
        source = lax.shift_right_logical(slot * 52429, 21)
        earlier = (owner == row) & (lane >= 40 * source) & (lane < slot)
        arrive = 2 * source + jnp.max(jnp.where(earlier, 1, 0), axis=1, keepdims=True)
        wanted = jnp.broadcast_to(mask[pl.ds(z, 1), :], (40, 1280))
        live = jnp.sum(jnp.where(lane == atom + 40 * row, wanted, 0), axis=1, keepdims=True)
        place = lane - 40 * row
        here = (owner == atom) & (place >= 0) & (place < 40)
        first = jnp.min(jnp.where(here, place, 39), axis=1, keepdims=True)
        last = jnp.max(jnp.where(here, place, 0), axis=1, keepdims=True)
        diagonal = lax.broadcasted_iota(jnp.int32, (40, 128), 1) == lax.broadcasted_iota(jnp.int32, (40, 128), 0)
        for r, value in enumerate((arrive, live, first, last)):
            table[r:r + 1, :] = jnp.sum(jnp.where(diagonal, value, 0), axis=0, keepdims=True)
        table[4:8, :] = jnp.zeros((4, 128), jnp.int32)
        to_scalar = pltpu.make_async_copy(table, table_s, load_sem.at[4])
        to_scalar.start()
        to_scalar.wait()

    def pack_and_send():
        build_tables()
        load_v.wait()
        for k in range(31):
            peer = peer_of(k)
            for s in range(2):
                vsend[2 * peer + s] = vin[table_s[2 + s, peer]]
            exchange(k).start()
        for s in range(2):
            vrecv[2 * row + s] = vin[table_s[2 + s, row]]

    def receive_blocks():
        all_of(vrecv.at[0:62], sent.at[0], a_recv.at[0]).wait_recv()

        def place(a, carry):
            live = jnp.full((32, 1024), table_s[1, a], jnp.int32).astype(F32).astype(BF)
            vord[pl.ds(pl.multiple_of(32 * a, 32), 32), :] = vrecv[table_s[0, a]] * live
            return carry

        lax.fori_loop(0, 40, place, 0)
        for k0, kw, c0, cw in ((0, 512, 0, 384), (512, 512, 384, 384), (1024, 256, 768, 128)):
            for n in range(4):
                vc[c0:c0 + cw, 256 * n:256 * n + 256] = jnp.dot(
                    smat[c0:c0 + cw, 0:kw], vord[k0:k0 + kw, 256 * n:256 * n + 256], preferred_element_type=F32
                ).astype(BF)
        vtail[...] = jnp.dot(smat[896:1088, 0:256], vord[1024:1280, :], preferred_element_type=F32).astype(BF)

    partner = row + 1 - 2 * core

    def pair_copy(p):
        return pltpu.make_async_remote_copy(
            src_ref=psend.at[p],
            dst_ref=prec.at[p],
            send_sem=sent.at[2],
            recv_sem=d_recv.at[p],
            device_id=(partner, z),
            device_id_type=MESH,
        )

    def product(p, qc, n):
        tiles = [gath[p, :, 7 * qc + t].reshape(256, 128) for t in range(7)] + [gath[p, :, 14].reshape(256, 128)]
        start = pl.multiple_of(64 * (1 - qc), 64)
        rhs = jnp.concatenate(
            [vc[:, 256 * n:256 * n + 256], vtail[pl.ds(start, 128), 256 * n:256 * n + 256]], axis=0
        )
        return jnp.dot(jnp.concatenate(tiles, axis=1), rhs, preferred_element_type=F32)

    def multiply(p):
        for n in range(4):
            psend[p, :, 256 * n:256 * n + 256] = product(p, 1 - core, n).astype(BF)
        pair_copy(p).start()
        for n in range(4):
            own[p, :, 256 * n:256 * n + 256] = product(p, core, n)

    def row_of(yy, xx):
        return (yy * 4 + xx) * 2 + core

    def first_copy(p, half, d):
        if half == 0:
            to = lax.rem(y + d, 4)
            src, dev = q.at[p, to, :, :, 0:512], row_of(to, x)
        else:
            to = lax.rem(x + d, 4)
            src, dev = q.at[p, :, to, :, 512:1024], row_of(y, to)
        return pltpu.make_async_remote_copy(
            src_ref=src,
            dst_ref=rb1.at[p, half, d - 1],
            send_sem=sent.at[3],
            recv_sem=s_recv.at[p],
            device_id=(dev, z),
            device_id_type=MESH,
        )

    def second_copy(p, half, d):
        if half == 0:
            to = lax.rem(x + d, 4)
            dev = row_of(y, to)
        else:
            to = lax.rem(y + d, 4)
            dev = row_of(to, x)
        return pltpu.make_async_remote_copy(
            src_ref=red.at[p, half, to],
            dst_ref=rb2.at[p, half, d - 1],
            send_sem=sent.at[4],
            recv_sem=t_recv.at[p],
            device_id=(dev, z),
            device_id_type=MESH,
        )

    def pair_sum(p):
        pair_copy(p).wait_recv()
        q[p] = (own[p] + prec[p].astype(F32)).astype(BF).reshape(4, 4, 16, 1024)
        for d in (2, 1, 3):
            for half in range(2):
                first_copy(p, half, d).start()

    def first_sum(p):
        all_of(rb1.at[p], sent.at[3], s_recv.at[p]).wait_recv()
        for half in range(2):
            mine = q[p, y, :, :, 0:512] if half == 0 else q[p, :, x, :, 512:1024]
            total = mine.astype(F32)
            for d in range(3):
                total = total + rb1[p, half, d].astype(F32)
            red[p, half] = total.astype(BF)
        for d in (2, 1, 3):
            for half in range(2):
                second_copy(p, half, d).start()

    def second_sum(p):
        all_of(rb2.at[p], sent.at[4], t_recv.at[p]).wait_recv()
        for half in range(2):
            total = red[p, half, x if half == 0 else y].astype(F32)
            for d in range(3):
                total = total + rb2[p, half, d].astype(F32)
            out_ref[16 * p:16 * p + 16, 512 * half:512 * half + 512] = total.astype(BF)

    packed = False
    for kind, p, h, side in build_schedule():
        if kind == "ring":
            if h > 1:
                if not packed:
                    pack_and_send()
                    packed = True
                ring_arrival(p, h - 1, side)
            ring(p, h, side).start()
        elif kind == "blocks":
            receive_blocks()
        elif kind == "multiply":
            for s in range(2):
                ring_arrival(p, hops(p)[s], s)
            multiply(p)
        elif kind == "pair":
            pair_sum(p)
        elif kind == "first":
            first_sum(p)
        else:
            second_sum(p)

    all_of(vsend.at[0:62], sent.at[0], a_recv.at[0]).wait_send()
    all_of(gath.at[0:7], sent.at[1], a_recv.at[0]).wait_send()
    all_of(psend, sent.at[2], a_recv.at[0]).wait_send()
    all_of(rb1, sent.at[3], a_recv.at[0]).wait_send()
    all_of(rb2, sent.at[4], a_recv.at[0]).wait_send()


def body(integrals, coeffs, mask, offsets, atom_of_slot):
    smem = pl.BlockSpec(memory_space=pltpu.SMEM)
    hbm = pl.BlockSpec(memory_space=pl.ANY)
    vmem = pltpu.VMEM
    dma = pltpu.SemaphoreType.DMA
    return pl.pallas_call(
        kernel,
        out_shape=jax.ShapeDtypeStruct((128, 1024), BF),
        in_specs=[smem, hbm, hbm, hbm, hbm],
        out_specs=pl.BlockSpec(memory_space=pltpu.VMEM),
        scratch_shapes=[
            vmem((1, 1280), jnp.int32),
            vmem((8, 1280), jnp.int32),
            vmem((8, 128), jnp.int32),
            pltpu.SMEM((8, 128), jnp.int32),
            vmem((40, 32, 1024), BF),
            vmem((1280, 512), BF),
            vmem((64, 32, 1024), BF),
            vmem((64, 32, 1024), BF),
            vmem((512, 1280), BF),
            vmem((1088, 512), BF),
            vmem((ROUNDS, 8, 15, 32, 128), BF),
            vmem((1280, 1024), BF),
            vmem((896, 1024), BF),
            vmem((192, 1024), BF),
            vmem((ROUNDS, 256, 1024), BF),
            vmem((ROUNDS, 256, 1024), F32),
            vmem((ROUNDS, 256, 1024), BF),
            vmem((ROUNDS, 4, 4, 16, 1024), BF),
            vmem((ROUNDS, 2, 3, 4, 16, 512), BF),
            vmem((ROUNDS, 2, 4, 16, 512), BF),
            vmem((ROUNDS, 2, 3, 16, 512), BF),
            dma((5,)),
            dma((5,)),
            dma((1,)),
            dma((len(RING_SEM),)),
            dma((ROUNDS,)),
            dma((ROUNDS,)),
            dma((ROUNDS,)),
        ],
        compiler_params=pltpu.CompilerParams(
            collective_id=0, has_side_effects=True, vmem_limit_bytes=66_000_000
        ),
    )(offsets, atom_of_slot.reshape(1, 1280), mask.T, coeffs, integrals)


def solution(mesh):
    in_specs = (P("row", None, "col"), P("row", "col"), P(), P(), P())
    return jax.shard_map(body, mesh=mesh, in_specs=in_specs, out_specs=P("row", "col"), check_vma=False)
```

```python
import functools

import jax
import jax.numpy as jnp
from jax import lax
from jax.experimental import pallas as pl
from jax.experimental.pallas import tpu as pltpu
from jax.sharding import PartitionSpec as P

MESH = pl.DeviceIdType.MESH
BF = jnp.bfloat16
F32 = jnp.float32

ROUNDS = 8
FAR = ((2, 2), (2, 0), (0, 2), (3, 2), (1, 2), (2, 3), (2, 1), (3, 1), (3, 3), (1, 3), (1, 1), (3, 0), (0, 3), (1, 0), (0, 1))

START = 5.5
SLOT = 2.65
WIRE = 2.4
V_READY = 55.5
LAG = 2


def hops(p):
    return (4, 3) if p % 4 < 2 else (3, 4)


RING_SEM = {
    key: n
    for n, key in enumerate(
        (side, p, h) for p in range(ROUNDS) for side in range(2) for h in range(1, hops(p)[side] + 1)
    )
}


def ring_slots(side):
    slot_of = {}
    slot = 0
    while len(slot_of) < sum(hops(p)[side] for p in range(ROUNDS)):
        for p in range(ROUNDS):
            h = 1
            while (p, h) in slot_of:
                h += 1
            if h <= hops(p)[side] and (h == 1 or slot_of[p, h - 1] + LAG <= slot):
                slot_of[p, h] = slot
                break
        slot += 1
    return slot_of


def build_schedule():
    slots = [ring_slots(side) for side in range(2)]
    landed = lambda p, h, side: START + (slots[side][p, h] + 1) * SLOT + WIRE
    pending = [(V_READY, 1, "blocks", 0, 0, 0)]
    for side in range(2):
        for (p, h), slot in slots[side].items():
            if h == 1:
                pending.append((START + max(0, slot - 2) * SLOT, 0, "ring", p, h, side))
            else:
                pending.append((landed(p, h - 1, side), 0, "ring", p, h, side))
    order, clock, links = [], START, 0.0
    have_blocks = False
    cost = {"ring": 0.02, "blocks": 0.8, "compact": 0.9, "theirs": 0.72, "mine": 0.7, "pair": 0.15, "first": 0.15, "second": 0.05}
    while pending:
        clock = max(clock, min(e[0] for e in pending))
        event = min((e for e in pending if e[0] <= clock), key=lambda e: (e[1], e[3], e[0], e[4]))
        pending.remove(event)
        order.append(event[2:])
        kind, p = event[2:4]
        clock += cost[kind]
        if kind == "blocks":
            pending.append((clock, 3, "compact", -1, 0, 0))
        elif kind == "compact":
            for p in range(ROUNDS):
                ready = max(landed(p, hops(p)[side], side) for side in range(2))
                pending.append((ready, 3 if p < ROUNDS - 2 else 1, "theirs", p, 0, 0))
        elif kind == "theirs":
            pending.append((clock, 3 if p < ROUNDS - 2 else 1, "mine", p, 0, 0))
        elif kind == "mine":
            pending.append((clock + (4.0 if p < ROUNDS - 1 else 1.6), 2, "pair", p, 0, 0))
        elif kind == "pair":
            links = max(links, clock) + 2.75
            pending.append((links + WIRE + 1.0, 2, "first", p, 0, 0))
        elif kind == "first":
            links = max(links, clock) + 0.7
            pending.append((links + WIRE + 0.5, 2, "second", p, 0, 0))
    return order


def kernel(
    off_s, holder_hbm, mask_hbm, coef_hbm, v_hbm, out_ref,
    holder, mask, table, table_s,
    vin, cin, vsend, vrecv, ct, smat, gath, vord, vc, vtail, psend, own, prec, q, rb1, red, rb2,
    load_sem, sent, a_recv, g_recv, d_recv, s_recv, t_recv,
):
    row = lax.axis_index("row")
    z = lax.axis_index("col")
    core = lax.rem(row, 2)
    chip = lax.div(row, 2)
    x = lax.rem(chip, 4)
    y = lax.div(chip, 4)
    zr = lax.rem(z + 1, 8)
    zl = lax.rem(z + 7, 8)

    load_c = pltpu.make_async_copy(coef_hbm, cin, load_sem.at[0])
    load_v = pltpu.make_async_copy(v_hbm, vin, load_sem.at[1])
    load_c.start()
    load_h = pltpu.make_async_copy(holder_hbm, holder, load_sem.at[2])
    load_m = pltpu.make_async_copy(mask_hbm, mask, load_sem.at[3])
    load_h.start()
    load_m.start()
    load_v.start()

    barrier = pltpu.get_barrier_semaphore()

    def greet(k, carry):
        peer = lax.rem(row + k, 32)
        pl.semaphore_signal(barrier, inc=1, device_id=(peer, z), device_id_type=MESH)
        return carry

    lax.fori_loop(1, 32, greet, 0)
    for side in (zr, zl):
        pl.semaphore_signal(barrier, inc=1, device_id=(row, side), device_id_type=MESH)

    m = lax.broadcasted_iota(jnp.int32, (48, 512), 0)
    k = lax.broadcasted_iota(jnp.int32, (48, 512), 1)
    for g in range(20):
        at = row * 40 + 2 * g
        length = off_s[at + 1] - off_s[at]
        src = jnp.where(m < length, m, 32 + m - length) + 64 * (g % 8)
        rows = jnp.where(k == src, 1.0, 0.0).astype(BF)
        if g < 18:
            smat[48 * g:48 * g + 48, :] = rows
        elif g == 18:
            smat[864:896, :] = rows[0:32]
            smat[960:976, :] = rows[32:48]
        else:
            smat[976:1024, :] = rows
    smat[896:960, :] = jnp.zeros((64, 512), BF)
    smat[1024:1088, :] = jnp.zeros((64, 512), BF)

    load_c.wait()
    rho = lax.broadcasted_iota(jnp.int32, (512, 512), 0)
    col = lax.broadcasted_iota(jnp.int32, (512, 512), 1)
    want = (rho & 15) + 256 * ((rho >> 4) & 1) + 16 * ((rho >> 5) & 7) + 128 * (rho >> 8)
    perm = jnp.where(col == want, 1.0, 0.0).astype(BF)
    for b in range(5):
        ct[:, 256 * b:256 * b + 256] = lax.dot_general(
            perm, cin[256 * b:256 * b + 256, :], (((1,), (1,)), ((), ())), preferred_element_type=F32
        ).astype(BF)

    def compact(r0, rw, k0, kw, c0, cw):
        return lax.dot_general(
            ct[r0:r0 + rw, k0:k0 + kw], smat[c0:c0 + cw, 0:kw], (((1,), (1,)), ((), ())), preferred_element_type=F32
        )

    for t0, k0, kw, c0, cw in ((0, 0, 512, 0, 384), (3, 512, 512, 384, 384), (6, 1024, 256, 768, 128)):
        piece = compact(0, 512, k0, kw, c0, cw).astype(BF).reshape(2, 8, 32, cw)
        for qc in range(2):
            for t in range(cw // 128):
                gath[:, z, 7 * qc + t0 + t] = piece[qc, :, :, 128 * t:128 * t + 128]
    tail = compact(0, 256, 1024, 256, 960, 128) + compact(256, 256, 1024, 256, 896, 128)
    gath[:, z, 14] = tail.astype(BF).reshape(8, 32, 128)

    pl.semaphore_wait(barrier, 33)

    def ring(p, h, side):
        src = lax.rem(z + (8 - (h - 1)), 8) if side == 0 else lax.rem(z + (h - 1), 8)
        return pltpu.make_async_remote_copy(
            src_ref=gath.at[p, src],
            dst_ref=gath.at[p, src],
            send_sem=sent.at[1],
            recv_sem=g_recv.at[RING_SEM[side, p, h]],
            device_id=(row, zr if side == 0 else zl),
            device_id_type=MESH,
        )

    def ring_arrival(p, h, side):
        src = lax.rem(z + (8 - h), 8) if side == 0 else lax.rem(z + h, 8)
        pltpu.make_async_remote_copy(
            src_ref=gath.at[p, src],
            dst_ref=gath.at[p, src],
            send_sem=sent.at[1],
            recv_sem=g_recv.at[RING_SEM[side, p, h]],
            device_id=(row, zr if side == 0 else zl),
            device_id_type=MESH,
        ).wait_recv()

    def place_of(k):
        if k == 30:
            return row + 1 - 2 * core
        dy, dx = FAR[k // 2]
        other = core if k % 2 == 0 else 1 - core
        return (lax.rem(y + dy, 4) * 4 + lax.rem(x + dx, 4)) * 2 + other

    def peer_of(k):
        return jnp.where(core == 0, place_of(k), place_of(30 - k))

    def exchange(k):
        peer = peer_of(k)
        return pltpu.make_async_remote_copy(
            src_ref=vsend.at[pl.ds(2 * peer, 2)],
            dst_ref=vrecv.at[pl.ds(2 * row, 2)],
            send_sem=sent.at[0],
            recv_sem=a_recv.at[0],
            device_id=(peer, z),
            device_id_type=MESH,
        )

    def all_of(ref, send_sem, recv_sem):
        return pltpu.make_async_remote_copy(
            src_ref=ref, dst_ref=ref, send_sem=send_sem, recv_sem=recv_sem,
            device_id=(row, zr), device_id_type=MESH,
        )

    def build_tables():
        load_h.wait()
        load_m.wait()
        lane = lax.broadcasted_iota(jnp.int32, (40, 1280), 1)
        atom = lax.broadcasted_iota(jnp.int32, (40, 1280), 0)
        held = jnp.concatenate([jnp.broadcast_to(holder[r:r + 1, :], (40, 128)) for r in range(10)], axis=1)
        owner = lax.shift_right_logical(held * 52429, 21)
        slot = jnp.max(jnp.where(held == atom + 40 * row, lane, 0), axis=1, keepdims=True)
        source = lax.shift_right_logical(slot * 52429, 21)
        earlier = (owner == row) & (lane >= 40 * source) & (lane < slot)
        arrive = 2 * source + jnp.max(jnp.where(earlier, 1, 0), axis=1, keepdims=True)
        wanted = jnp.broadcast_to(mask[pl.ds(z, 1), :], (40, 1280))
        live = jnp.sum(jnp.where(lane == atom + 40 * row, wanted, 0), axis=1, keepdims=True)
        place = lane - 40 * row
        here = (owner == atom) & (place >= 0) & (place < 40)
        first = jnp.min(jnp.where(here, place, 39), axis=1, keepdims=True)
        last = jnp.max(jnp.where(here, place, 0), axis=1, keepdims=True)
        diagonal = lax.broadcasted_iota(jnp.int32, (40, 128), 1) == lax.broadcasted_iota(jnp.int32, (40, 128), 0)
        for r, value in enumerate((arrive, live, first, last)):
            table[r:r + 1, :] = jnp.sum(jnp.where(diagonal, value, 0), axis=0, keepdims=True)
        table[4:8, :] = jnp.zeros((4, 128), jnp.int32)
        to_scalar = pltpu.make_async_copy(table, table_s, load_sem.at[4])
        to_scalar.start()
        to_scalar.wait()

    def pack_and_send():
        build_tables()
        load_v.wait()
        for k in range(31):
            peer = peer_of(k)
            for s in range(2):
                vsend[2 * peer + s] = vin[table_s[2 + s, peer]]
            exchange(k).start()
        for s in range(2):
            vrecv[2 * row + s] = vin[table_s[2 + s, row]]

    def receive_blocks():
        all_of(vrecv.at[0:62], sent.at[0], a_recv.at[0]).wait_recv()

        def place(a, carry):
            live = jnp.full((32, 1024), table_s[1, a], jnp.int32).astype(F32).astype(BF)
            vord[pl.ds(pl.multiple_of(32 * a, 32), 32), :] = vrecv[table_s[0, a]] * live
            return carry

        lax.fori_loop(0, 40, place, 0)

    def compact_blocks():
        for k0, kw, c0, cw in ((0, 512, 0, 384), (512, 512, 384, 384), (1024, 256, 768, 128)):
            for n in range(4):
                vc[c0:c0 + cw, 256 * n:256 * n + 256] = jnp.dot(
                    smat[c0:c0 + cw, 0:kw], vord[k0:k0 + kw, 256 * n:256 * n + 256], preferred_element_type=F32
                ).astype(BF)
        vtail[...] = jnp.dot(smat[896:1088, 0:256], vord[1024:1280, :], preferred_element_type=F32).astype(BF)

    partner = row + 1 - 2 * core

    def pair_copy(p):
        return pltpu.make_async_remote_copy(
            src_ref=psend.at[p],
            dst_ref=prec.at[p],
            send_sem=sent.at[2],
            recv_sem=d_recv.at[p],
            device_id=(partner, z),
            device_id_type=MESH,
        )

    def product(p, qc, n):
        tiles = [gath[p, :, 7 * qc + t].reshape(256, 128) for t in range(7)] + [gath[p, :, 14].reshape(256, 128)]
        start = pl.multiple_of(64 * (1 - qc), 64)
        rhs = jnp.concatenate(
            [vc[:, 256 * n:256 * n + 256], vtail[pl.ds(start, 128), 256 * n:256 * n + 256]], axis=0
        )
        return jnp.dot(jnp.concatenate(tiles, axis=1), rhs, preferred_element_type=F32)

    def multiply_theirs(p):
        for n in range(4):
            psend[p, :, 256 * n:256 * n + 256] = product(p, 1 - core, n).astype(BF)
        pair_copy(p).start()

    def multiply_mine(p):
        for n in range(4):
            own[p, :, 256 * n:256 * n + 256] = product(p, core, n)

    def row_of(yy, xx):
        return (yy * 4 + xx) * 2 + core

    def first_copy(p, half, d):
        if half == 0:
            to = lax.rem(y + d, 4)
            src, dev = q.at[p, to, :, :, 0:512], row_of(to, x)
        else:
            to = lax.rem(x + d, 4)
            src, dev = q.at[p, :, to, :, 512:1024], row_of(y, to)
        return pltpu.make_async_remote_copy(
            src_ref=src,
            dst_ref=rb1.at[p, half, d - 1],
            send_sem=sent.at[3],
            recv_sem=s_recv.at[p],
            device_id=(dev, z),
            device_id_type=MESH,
        )

    def second_copy(p, half, d):
        if half == 0:
            to = lax.rem(x + d, 4)
            dev = row_of(y, to)
        else:
            to = lax.rem(y + d, 4)
            dev = row_of(to, x)
        return pltpu.make_async_remote_copy(
            src_ref=red.at[p, half, to],
            dst_ref=rb2.at[p, half, d - 1],
            send_sem=sent.at[4],
            recv_sem=t_recv.at[p],
            device_id=(dev, z),
            device_id_type=MESH,
        )

    def pair_sum(p):
        pair_copy(p).wait_recv()
        q[p] = (own[p] + prec[p].astype(F32)).astype(BF).reshape(4, 4, 16, 1024)
        for d in (2, 1, 3):
            for half in range(2):
                first_copy(p, half, d).start()

    def first_sum(p):
        all_of(rb1.at[p], sent.at[3], s_recv.at[p]).wait_recv()
        for half in range(2):
            mine = q[p, y, :, :, 0:512] if half == 0 else q[p, :, x, :, 512:1024]
            total = mine.astype(F32)
            for d in range(3):
                total = total + rb1[p, half, d].astype(F32)
            red[p, half] = total.astype(BF)
        for d in (2, 1, 3):
            for half in range(2):
                second_copy(p, half, d).start()

    def second_sum(p):
        all_of(rb2.at[p], sent.at[4], t_recv.at[p]).wait_recv()
        for half in range(2):
            total = red[p, half, x if half == 0 else y].astype(F32)
            for d in range(3):
                total = total + rb2[p, half, d].astype(F32)
            out_ref[16 * p:16 * p + 16, 512 * half:512 * half + 512] = total.astype(BF)

    packed = False
    for kind, p, h, side in build_schedule():
        if kind == "ring":
            if h > 1:
                if not packed:
                    pack_and_send()
                    packed = True
                ring_arrival(p, h - 1, side)
            ring(p, h, side).start()
        elif kind == "blocks":
            receive_blocks()
        elif kind == "compact":
            compact_blocks()
        elif kind == "theirs":
            for s in range(2):
                ring_arrival(p, hops(p)[s], s)
            multiply_theirs(p)
        elif kind == "mine":
            multiply_mine(p)
        elif kind == "pair":
            pair_sum(p)
        elif kind == "first":
            first_sum(p)
        else:
            second_sum(p)

    all_of(vsend.at[0:62], sent.at[0], a_recv.at[0]).wait_send()
    all_of(gath.at[0:7], sent.at[1], a_recv.at[0]).wait_send()
    all_of(psend, sent.at[2], a_recv.at[0]).wait_send()
    all_of(rb1, sent.at[3], a_recv.at[0]).wait_send()
    all_of(rb2, sent.at[4], a_recv.at[0]).wait_send()


def body(integrals, coeffs, mask, offsets, atom_of_slot):
    smem = pl.BlockSpec(memory_space=pltpu.SMEM)
    hbm = pl.BlockSpec(memory_space=pl.ANY)
    vmem = pltpu.VMEM
    dma = pltpu.SemaphoreType.DMA
    return pl.pallas_call(
        kernel,
        out_shape=pltpu.VMEM((128, 1024), BF),
        in_specs=[smem, hbm, hbm, hbm, hbm],
        out_specs=pl.BlockSpec(memory_space=pltpu.VMEM),
        scratch_shapes=[
            vmem((10, 128), jnp.int32),
            vmem((8, 1280), jnp.int32),
            vmem((8, 128), jnp.int32),
            pltpu.SMEM((8, 128), jnp.int32),
            vmem((40, 32, 1024), BF),
            vmem((1280, 512), BF),
            vmem((64, 32, 1024), BF),
            vmem((64, 32, 1024), BF),
            vmem((512, 1280), BF),
            vmem((1088, 512), BF),
            vmem((ROUNDS, 8, 15, 32, 128), BF),
            vmem((1280, 1024), BF),
            vmem((896, 1024), BF),
            vmem((192, 1024), BF),
            vmem((ROUNDS, 256, 1024), BF),
            vmem((ROUNDS, 256, 1024), F32),
            vmem((ROUNDS, 256, 1024), BF),
            vmem((ROUNDS, 4, 4, 16, 1024), BF),
            vmem((ROUNDS, 2, 3, 4, 16, 512), BF),
            vmem((ROUNDS, 2, 4, 16, 512), BF),
            vmem((ROUNDS, 2, 3, 16, 512), BF),
            dma((5,)),
            dma((5,)),
            dma((1,)),
            dma((len(RING_SEM),)),
            dma((ROUNDS,)),
            dma((ROUNDS,)),
            dma((ROUNDS,)),
        ],
        compiler_params=pltpu.CompilerParams(
            collective_id=0, has_side_effects=True, vmem_limit_bytes=60_000_000
        ),
    )(offsets, atom_of_slot.reshape(10, 128), mask.T, coeffs, integrals)


def solution(mesh):
    in_specs = (P("row", None, "col"), P("row", "col"), P(), P(), P())
    return jax.shard_map(body, mesh=mesh, in_specs=in_specs, out_specs=P("row", "col"), check_vma=False)
```

```python
import functools

import jax
import jax.numpy as jnp
from jax import lax
from jax.experimental import pallas as pl
from jax.experimental.pallas import tpu as pltpu
from jax.sharding import PartitionSpec as P

MESH = pl.DeviceIdType.MESH
BF = jnp.bfloat16
F32 = jnp.float32

ROUNDS = 8
FAR = ((2, 2), (2, 0), (0, 2), (3, 2), (1, 2), (2, 3), (2, 1), (3, 1), (3, 3), (1, 3), (1, 1), (3, 0), (0, 3), (1, 0), (0, 1))

START = 5.5
SLOT = 2.65
WIRE = 2.4
V_READY = 55.5
LAG = 2


def hops(p):
    return (4, 3) if p % 4 < 2 else (3, 4)


RING_SEM = {
    key: n
    for n, key in enumerate(
        (side, p, h) for p in range(ROUNDS) for side in range(2) for h in range(1, hops(p)[side] + 1)
    )
}


def ring_slots(side):
    slot_of = {}
    slot = 0
    while len(slot_of) < sum(hops(p)[side] for p in range(ROUNDS)):
        for p in range(ROUNDS):
            h = 1
            while (p, h) in slot_of:
                h += 1
            if h <= hops(p)[side] and (h == 1 or slot_of[p, h - 1] + LAG <= slot):
                slot_of[p, h] = slot
                break
        slot += 1
    return slot_of


def build_schedule():
    slots = [ring_slots(side) for side in range(2)]
    landed = lambda p, h, side: START + (slots[side][p, h] + 1) * SLOT + WIRE
    pending = [(V_READY, 1, "blocks", 0, 0, 0)]
    for side in range(2):
        for (p, h), slot in slots[side].items():
            if h == 1:
                pending.append((START + max(0, slot - 2) * SLOT, 0, "ring", p, h, side))
            else:
                pending.append((landed(p, h - 1, side), 0, "ring", p, h, side))
    order, clock, links = [], START, 0.0
    have_blocks = False
    cost = {"ring": 0.02, "blocks": 0.8, "compact": 0.9, "theirs": 0.72, "mine": 0.7, "pair": 0.15, "first": 0.15, "second": 0.05}
    while pending:
        clock = max(clock, min(e[0] for e in pending))
        event = min((e for e in pending if e[0] <= clock), key=lambda e: (e[1], e[3], e[0], e[4]))
        pending.remove(event)
        order.append(event[2:])
        kind, p = event[2:4]
        clock += cost[kind]
        if kind == "blocks":
            pending.append((clock, 3, "compact", -1, 0, 0))
        elif kind == "compact":
            for p in range(ROUNDS):
                ready = max(landed(p, hops(p)[side], side) for side in range(2))
                pending.append((ready, 3 if p < ROUNDS - 2 else 1, "theirs", p, 0, 0))
        elif kind == "theirs":
            pending.append((clock, 3 if p < ROUNDS - 2 else 1, "mine", p, 0, 0))
        elif kind == "mine":
            pending.append((clock + (4.0 if p < ROUNDS - 1 else 1.6), 2, "pair", p, 0, 0))
        elif kind == "pair":
            links = max(links, clock) + 2.75
            pending.append((links + WIRE + 1.0, 2, "first", p, 0, 0))
        elif kind == "first":
            links = max(links, clock) + 0.7
            pending.append((links + WIRE + 0.5, 2, "second", p, 0, 0))
    return order


def kernel(
    off_s, holder_hbm, mask_hbm, coef_hbm, v_hbm, out_ref,
    holder, mask, table, table_s,
    vin, cin, vsend, vrecv, ct, smat, gath, vord, vc, vtail, psend, own, prec, q, rb1, red, rb2,
    load_sem, sent, a_recv, g_recv, d_recv, s_recv, t_recv,
):
    row = lax.axis_index("row")
    z = lax.axis_index("col")
    core = lax.rem(row, 2)
    chip = lax.div(row, 2)
    x = lax.rem(chip, 4)
    y = lax.div(chip, 4)
    zr = lax.rem(z + 1, 8)
    zl = lax.rem(z + 7, 8)

    load_c = pltpu.make_async_copy(coef_hbm, cin, load_sem.at[0])
    load_v = pltpu.make_async_copy(v_hbm, vin, load_sem.at[1])
    load_c.start()
    load_h = pltpu.make_async_copy(holder_hbm, holder, load_sem.at[2])
    load_m = pltpu.make_async_copy(mask_hbm, mask, load_sem.at[3])
    load_h.start()
    load_m.start()

    barrier = pltpu.get_barrier_semaphore()

    def greet(k, carry):
        peer = lax.rem(row + k, 32)
        pl.semaphore_signal(barrier, inc=1, device_id=(peer, z), device_id_type=MESH)
        return carry

    lax.fori_loop(1, 32, greet, 0)
    for side in (zr, zl):
        pl.semaphore_signal(barrier, inc=1, device_id=(row, side), device_id_type=MESH)

    m = lax.broadcasted_iota(jnp.int32, (48, 512), 0)
    k = lax.broadcasted_iota(jnp.int32, (48, 512), 1)
    for g in range(20):
        at = row * 40 + 2 * g
        length = off_s[at + 1] - off_s[at]
        src = jnp.where(m < length, m, 32 + m - length) + 64 * (g % 8)
        rows = jnp.where(k == src, 1.0, 0.0).astype(BF)
        if g < 18:
            smat[48 * g:48 * g + 48, :] = rows
        elif g == 18:
            smat[864:896, :] = rows[0:32]
            smat[960:976, :] = rows[32:48]
        else:
            smat[976:1024, :] = rows
    smat[896:960, :] = jnp.zeros((64, 512), BF)
    smat[1024:1088, :] = jnp.zeros((64, 512), BF)

    one = lax.broadcasted_iota(jnp.int32, (256, 256), 0) == lax.broadcasted_iota(jnp.int32, (256, 256), 1)
    eye = jnp.where(one, 1.0, 0.0).astype(BF)

    load_c.wait()
    load_v.start()
    for b in range(5):
        for half in range(2):
            turned = lax.dot_general(
                eye, cin[256 * b:256 * b + 256, 256 * half:256 * half + 256],
                (((1,), (1,)), ((), ())), preferred_element_type=F32,
            ).astype(BF)
            for qc in range(2):
                for p in range(ROUNDS):
                    at = 256 * qc + 32 * p + 16 * half
                    ct[at:at + 16, 256 * b:256 * b + 256] = turned[128 * qc + 16 * p:128 * qc + 16 * p + 16, :]

    def compact(r0, rw, k0, kw, c0, cw):
        return lax.dot_general(
            ct[r0:r0 + rw, k0:k0 + kw], smat[c0:c0 + cw, 0:kw], (((1,), (1,)), ((), ())), preferred_element_type=F32
        )

    for t0, k0, kw, c0, cw in ((0, 0, 512, 0, 384), (3, 512, 512, 384, 384), (6, 1024, 256, 768, 128)):
        piece = compact(0, 512, k0, kw, c0, cw).astype(BF).reshape(2, 8, 32, cw)
        for qc in range(2):
            for t in range(cw // 128):
                gath[:, z, 7 * qc + t0 + t] = piece[qc, :, :, 128 * t:128 * t + 128]
    tail = compact(0, 256, 1024, 256, 960, 128) + compact(256, 256, 1024, 256, 896, 128)
    gath[:, z, 14] = tail.astype(BF).reshape(8, 32, 128)

    pl.semaphore_wait(barrier, 33)

    def ring(p, h, side):
        src = lax.rem(z + (8 - (h - 1)), 8) if side == 0 else lax.rem(z + (h - 1), 8)
        return pltpu.make_async_remote_copy(
            src_ref=gath.at[p, src],
            dst_ref=gath.at[p, src],
            send_sem=sent.at[1],
            recv_sem=g_recv.at[RING_SEM[side, p, h]],
            device_id=(row, zr if side == 0 else zl),
            device_id_type=MESH,
        )

    def ring_arrival(p, h, side):
        src = lax.rem(z + (8 - h), 8) if side == 0 else lax.rem(z + h, 8)
        pltpu.make_async_remote_copy(
            src_ref=gath.at[p, src],
            dst_ref=gath.at[p, src],
            send_sem=sent.at[1],
            recv_sem=g_recv.at[RING_SEM[side, p, h]],
            device_id=(row, zr if side == 0 else zl),
            device_id_type=MESH,
        ).wait_recv()

    def place_of(k):
        if k == 30:
            return row + 1 - 2 * core
        dy, dx = FAR[k // 2]
        other = core if k % 2 == 0 else 1 - core
        return (lax.rem(y + dy, 4) * 4 + lax.rem(x + dx, 4)) * 2 + other

    def peer_of(k):
        return jnp.where(core == 0, place_of(k), place_of(30 - k))

    def exchange(k):
        peer = peer_of(k)
        return pltpu.make_async_remote_copy(
            src_ref=vsend.at[pl.ds(2 * peer, 2)],
            dst_ref=vrecv.at[pl.ds(2 * row, 2)],
            send_sem=sent.at[0],
            recv_sem=a_recv.at[0],
            device_id=(peer, z),
            device_id_type=MESH,
        )

    def all_of(ref, send_sem, recv_sem):
        return pltpu.make_async_remote_copy(
            src_ref=ref, dst_ref=ref, send_sem=send_sem, recv_sem=recv_sem,
            device_id=(row, zr), device_id_type=MESH,
        )

    def build_tables():
        load_h.wait()
        load_m.wait()
        lane = lax.broadcasted_iota(jnp.int32, (40, 1280), 1)
        atom = lax.broadcasted_iota(jnp.int32, (40, 1280), 0)
        held = jnp.concatenate([jnp.broadcast_to(holder[r:r + 1, :], (40, 128)) for r in range(10)], axis=1)
        owner = lax.shift_right_logical(held * 52429, 21)
        slot = jnp.max(jnp.where(held == atom + 40 * row, lane, 0), axis=1, keepdims=True)
        source = lax.shift_right_logical(slot * 52429, 21)
        earlier = (owner == row) & (lane >= 40 * source) & (lane < slot)
        arrive = 2 * source + jnp.max(jnp.where(earlier, 1, 0), axis=1, keepdims=True)
        wanted = jnp.broadcast_to(mask[pl.ds(z, 1), :], (40, 1280))
        live = jnp.sum(jnp.where(lane == atom + 40 * row, wanted, 0), axis=1, keepdims=True)
        place = lane - 40 * row
        here = (owner == atom) & (place >= 0) & (place < 40)
        first = jnp.min(jnp.where(here, place, 39), axis=1, keepdims=True)
        last = jnp.max(jnp.where(here, place, 0), axis=1, keepdims=True)
        diagonal = lax.broadcasted_iota(jnp.int32, (40, 128), 1) == lax.broadcasted_iota(jnp.int32, (40, 128), 0)
        for r, value in enumerate((arrive, live, first, last)):
            table[r:r + 1, :] = jnp.sum(jnp.where(diagonal, value, 0), axis=0, keepdims=True)
        table[4:8, :] = jnp.zeros((4, 128), jnp.int32)
        to_scalar = pltpu.make_async_copy(table, table_s, load_sem.at[4])
        to_scalar.start()
        to_scalar.wait()

    def pack_and_send():
        build_tables()
        load_v.wait()
        for k in range(31):
            peer = peer_of(k)
            for s in range(2):
                vsend[2 * peer + s] = vin[table_s[2 + s, peer]]
            exchange(k).start()
        for s in range(2):
            vrecv[2 * row + s] = vin[table_s[2 + s, row]]

    def receive_blocks():
        all_of(vrecv.at[0:62], sent.at[0], a_recv.at[0]).wait_recv()

        def place(a, carry):
            live = jnp.full((32, 1024), table_s[1, a], jnp.int32).astype(F32).astype(BF)
            vord[pl.ds(pl.multiple_of(32 * a, 32), 32), :] = vrecv[table_s[0, a]] * live
            return carry

        lax.fori_loop(0, 40, place, 0)

    def compact_blocks():
        for k0, kw, c0, cw in ((0, 512, 0, 384), (512, 512, 384, 384), (1024, 256, 768, 128)):
            for n in range(4):
                vc[c0:c0 + cw, 256 * n:256 * n + 256] = jnp.dot(
                    smat[c0:c0 + cw, 0:kw], vord[k0:k0 + kw, 256 * n:256 * n + 256], preferred_element_type=F32
                ).astype(BF)
        vtail[...] = jnp.dot(smat[896:1088, 0:256], vord[1024:1280, :], preferred_element_type=F32).astype(BF)

    partner = row + 1 - 2 * core

    def pair_copy(p):
        return pltpu.make_async_remote_copy(
            src_ref=psend.at[p],
            dst_ref=prec.at[p],
            send_sem=sent.at[2],
            recv_sem=d_recv.at[p],
            device_id=(partner, z),
            device_id_type=MESH,
        )

    def product(p, qc, n):
        tiles = [gath[p, :, 7 * qc + t].reshape(256, 128) for t in range(7)] + [gath[p, :, 14].reshape(256, 128)]
        start = pl.multiple_of(64 * (1 - qc), 64)
        rhs = jnp.concatenate(
            [vc[:, 256 * n:256 * n + 256], vtail[pl.ds(start, 128), 256 * n:256 * n + 256]], axis=0
        )
        return jnp.dot(jnp.concatenate(tiles, axis=1), rhs, preferred_element_type=F32)

    def multiply_theirs(p):
        for n in range(4):
            psend[p, :, 256 * n:256 * n + 256] = product(p, 1 - core, n).astype(BF)
        pair_copy(p).start()

    def multiply_mine(p):
        for n in range(4):
            own[p, :, 256 * n:256 * n + 256] = product(p, core, n)

    def row_of(yy, xx):
        return (yy * 4 + xx) * 2 + core

    def first_copy(p, half, d):
        if half == 0:
            to = lax.rem(y + d, 4)
            src, dev = q.at[p, to, :, :, 0:512], row_of(to, x)
        else:
            to = lax.rem(x + d, 4)
            src, dev = q.at[p, :, to, :, 512:1024], row_of(y, to)
        return pltpu.make_async_remote_copy(
            src_ref=src,
            dst_ref=rb1.at[p, half, d - 1],
            send_sem=sent.at[3],
            recv_sem=s_recv.at[p],
            device_id=(dev, z),
            device_id_type=MESH,
        )

    def second_copy(p, half, d):
        if half == 0:
            to = lax.rem(x + d, 4)
            dev = row_of(y, to)
        else:
            to = lax.rem(y + d, 4)
            dev = row_of(to, x)
        return pltpu.make_async_remote_copy(
            src_ref=red.at[p, half, to],
            dst_ref=rb2.at[p, half, d - 1],
            send_sem=sent.at[4],
            recv_sem=t_recv.at[p],
            device_id=(dev, z),
            device_id_type=MESH,
        )

    def pair_sum(p):
        pair_copy(p).wait_recv()
        q[p] = (own[p] + prec[p].astype(F32)).astype(BF).reshape(4, 4, 16, 1024)
        for d in (2, 1, 3):
            for half in range(2):
                first_copy(p, half, d).start()

    def first_sum(p):
        all_of(rb1.at[p], sent.at[3], s_recv.at[p]).wait_recv()
        for half in range(2):
            mine = q[p, y, :, :, 0:512] if half == 0 else q[p, :, x, :, 512:1024]
            total = mine.astype(F32)
            for d in range(3):
                total = total + rb1[p, half, d].astype(F32)
            red[p, half] = total.astype(BF)
        for d in (2, 1, 3):
            for half in range(2):
                second_copy(p, half, d).start()

    def second_sum(p):
        all_of(rb2.at[p], sent.at[4], t_recv.at[p]).wait_recv()
        for half in range(2):
            total = red[p, half, x if half == 0 else y].astype(F32)
            for d in range(3):
                total = total + rb2[p, half, d].astype(F32)
            out_ref[16 * p:16 * p + 16, 512 * half:512 * half + 512] = total.astype(BF)

    packed = False
    for kind, p, h, side in build_schedule():
        if kind == "ring":
            if h > 1:
                if not packed:
                    pack_and_send()
                    packed = True
                ring_arrival(p, h - 1, side)
            ring(p, h, side).start()
        elif kind == "blocks":
            receive_blocks()
        elif kind == "compact":
            compact_blocks()
        elif kind == "theirs":
            for s in range(2):
                ring_arrival(p, hops(p)[s], s)
            multiply_theirs(p)
        elif kind == "mine":
            multiply_mine(p)
        elif kind == "pair":
            pair_sum(p)
        elif kind == "first":
            first_sum(p)
        else:
            second_sum(p)

    all_of(vsend.at[0:62], sent.at[0], a_recv.at[0]).wait_send()
    all_of(gath.at[0:7], sent.at[1], a_recv.at[0]).wait_send()
    all_of(psend, sent.at[2], a_recv.at[0]).wait_send()
    all_of(rb1, sent.at[3], a_recv.at[0]).wait_send()
    all_of(rb2, sent.at[4], a_recv.at[0]).wait_send()


def body(integrals, coeffs, mask, offsets, atom_of_slot):
    smem = pl.BlockSpec(memory_space=pltpu.SMEM)
    hbm = pl.BlockSpec(memory_space=pl.ANY)
    vmem = pltpu.VMEM
    dma = pltpu.SemaphoreType.DMA
    return pl.pallas_call(
        kernel,
        out_shape=pltpu.VMEM((128, 1024), BF),
        in_specs=[smem, hbm, hbm, hbm, hbm],
        out_specs=pl.BlockSpec(memory_space=pltpu.VMEM),
        scratch_shapes=[
            vmem((10, 128), jnp.int32),
            vmem((8, 1280), jnp.int32),
            vmem((8, 128), jnp.int32),
            pltpu.SMEM((8, 128), jnp.int32),
            vmem((40, 32, 1024), BF),
            vmem((1280, 512), BF),
            vmem((64, 32, 1024), BF),
            vmem((64, 32, 1024), BF),
            vmem((512, 1280), BF),
            vmem((1088, 512), BF),
            vmem((ROUNDS, 8, 15, 32, 128), BF),
            vmem((1280, 1024), BF),
            vmem((896, 1024), BF),
            vmem((192, 1024), BF),
            vmem((ROUNDS, 256, 1024), BF),
            vmem((ROUNDS, 256, 1024), F32),
            vmem((ROUNDS, 256, 1024), BF),
            vmem((ROUNDS, 4, 4, 16, 1024), BF),
            vmem((ROUNDS, 2, 3, 4, 16, 512), BF),
            vmem((ROUNDS, 2, 4, 16, 512), BF),
            vmem((ROUNDS, 2, 3, 16, 512), BF),
            dma((5,)),
            dma((5,)),
            dma((1,)),
            dma((len(RING_SEM),)),
            dma((ROUNDS,)),
            dma((ROUNDS,)),
            dma((ROUNDS,)),
        ],
        compiler_params=pltpu.CompilerParams(
            collective_id=0, has_side_effects=True, vmem_limit_bytes=60_000_000
        ),
    )(offsets, atom_of_slot.reshape(10, 128), mask.T, coeffs, integrals)


def solution(mesh):
    in_specs = (P("row", None, "col"), P("row", "col"), P(), P(), P())
    return jax.shard_map(body, mesh=mesh, in_specs=in_specs, out_specs=P("row", "col"), check_vma=False)
```

```python
import functools

import jax
import jax.numpy as jnp
from jax import lax
from jax.experimental import pallas as pl
from jax.experimental.pallas import tpu as pltpu
from jax.sharding import PartitionSpec as P

MESH = pl.DeviceIdType.MESH
BF = jnp.bfloat16
F32 = jnp.float32

ROUNDS = 8
FAR = ((2, 2), (2, 0), (0, 2), (3, 2), (1, 2), (2, 3), (2, 1), (3, 1), (3, 3), (1, 3), (1, 1), (3, 0), (0, 3), (1, 0), (0, 1))

START = 5.5
SLOT = 2.65
WIRE = 2.4
V_READY = 56.3
LAG = 2


def hops(p):
    return (4, 3) if p % 4 < 2 else (3, 4)


RING_SEM = {
    key: n
    for n, key in enumerate(
        (side, p, h) for p in range(ROUNDS) for side in range(2) for h in range(1, hops(p)[side] + 1)
    )
}


def ring_slots(side):
    slot_of = {}
    slot = 0
    while len(slot_of) < sum(hops(p)[side] for p in range(ROUNDS)):
        for p in range(ROUNDS):
            h = 1
            while (p, h) in slot_of:
                h += 1
            if h <= hops(p)[side] and (h == 1 or slot_of[p, h - 1] + LAG <= slot):
                slot_of[p, h] = slot
                break
        slot += 1
    return slot_of


def build_schedule():
    slots = [ring_slots(side) for side in range(2)]
    landed = lambda p, h, side: START + (slots[side][p, h] + 1) * SLOT + WIRE
    pending = [(V_READY, 1, "blocks", 0, 0, 0)]
    for side in range(2):
        for (p, h), slot in slots[side].items():
            if h == 1:
                pending.append((START + max(0, slot - 2) * SLOT, 0, "ring", p, h, side))
            else:
                pending.append((landed(p, h - 1, side), 0, "ring", p, h, side))
    order, clock, links = [], START, 0.0
    have_blocks = False
    cost = {"ring": 0.02, "blocks": 0.8, "compact": 0.9, "theirs": 0.72, "mine": 0.7, "pair": 0.15, "first": 0.15, "second": 0.05}
    while pending:
        clock = max(clock, min(e[0] for e in pending))
        event = min((e for e in pending if e[0] <= clock), key=lambda e: (e[1], e[3], e[0], e[4]))
        pending.remove(event)
        order.append(event[2:])
        kind, p = event[2:4]
        clock += cost[kind]
        if kind == "blocks":
            pending.append((clock, 3, "compact", -1, 0, 0))
        elif kind == "compact":
            for p in range(ROUNDS):
                ready = max(landed(p, hops(p)[side], side) for side in range(2))
                pending.append((ready, 3 if p < ROUNDS - 2 else 1, "theirs", p, 0, 0))
        elif kind == "theirs":
            pending.append((clock, 3 if p < ROUNDS - 2 else 1, "mine", p, 0, 0))
        elif kind == "mine":
            pending.append((clock + (4.0 if p < ROUNDS - 1 else 1.6), 2, "pair", p, 0, 0))
        elif kind == "pair":
            links = max(links, clock) + 2.75
            pending.append((links + WIRE + 1.0, 2, "first", p, 0, 0))
        elif kind == "first":
            links = max(links, clock) + 0.7
            pending.append((links + WIRE + 0.5, 2, "second", p, 0, 0))
    return order


def kernel(
    off_s, holder_hbm, mask_hbm, coef_hbm, v_hbm, out_ref,
    holder, mask, table, table_s,
    vin, cin, vsend, vrecv, ct, smat, gath, vord, vc, vtail, psend, own, prec, q, rb1, red, rb2,
    load_sem, sent, a_recv, g_recv, d_recv, s_recv, t_recv,
):
    row = lax.axis_index("row")
    z = lax.axis_index("col")
    core = lax.rem(row, 2)
    chip = lax.div(row, 2)
    x = lax.rem(chip, 4)
    y = lax.div(chip, 4)
    zr = lax.rem(z + 1, 8)
    zl = lax.rem(z + 7, 8)

    load_c = pltpu.make_async_copy(coef_hbm, cin, load_sem.at[0])
    load_v = pltpu.make_async_copy(v_hbm, vin, load_sem.at[1])
    load_c.start()
    load_h = pltpu.make_async_copy(holder_hbm, holder, load_sem.at[2])
    load_m = pltpu.make_async_copy(mask_hbm, mask, load_sem.at[3])
    load_h.start()
    load_m.start()

    barrier = pltpu.get_barrier_semaphore()

    def greet(k, carry):
        peer = lax.rem(row + k, 32)
        pl.semaphore_signal(barrier, inc=1, device_id=(peer, z), device_id_type=MESH)
        return carry

    lax.fori_loop(1, 32, greet, 0)
    for side in (zr, zl):
        pl.semaphore_signal(barrier, inc=1, device_id=(row, side), device_id_type=MESH)

    m = lax.broadcasted_iota(jnp.int32, (48, 512), 0)
    k = lax.broadcasted_iota(jnp.int32, (48, 512), 1)
    for g in range(20):
        at = row * 40 + 2 * g
        length = off_s[at + 1] - off_s[at]
        src = jnp.where(m < length, m, 32 + m - length) + 64 * (g % 8)
        rows = jnp.where(k == src, 1.0, 0.0).astype(BF)
        if g < 18:
            smat[48 * g:48 * g + 48, :] = rows
        elif g == 18:
            smat[864:896, :] = rows[0:32]
            smat[960:976, :] = rows[32:48]
        else:
            smat[976:1024, :] = rows
    smat[896:960, :] = jnp.zeros((64, 512), BF)
    smat[1024:1088, :] = jnp.zeros((64, 512), BF)

    one = lax.broadcasted_iota(jnp.int32, (256, 256), 0) == lax.broadcasted_iota(jnp.int32, (256, 256), 1)
    eye = jnp.where(one, 1.0, 0.0).astype(BF)

    load_c.wait()
    load_v.start()
    for b in range(5):
        for half in range(2):
            turned = lax.dot_general(
                eye, cin[256 * b:256 * b + 256, 256 * half:256 * half + 256],
                (((1,), (1,)), ((), ())), preferred_element_type=F32,
            ).astype(BF)
            for qc in range(2):
                for p in range(ROUNDS):
                    at = 256 * qc + 32 * p + 16 * half
                    ct[at:at + 16, 256 * b:256 * b + 256] = turned[128 * qc + 16 * p:128 * qc + 16 * p + 16, :]

    def compact(r0, rw, k0, kw, c0, cw):
        return lax.dot_general(
            ct[r0:r0 + rw, k0:k0 + kw], smat[c0:c0 + cw, 0:kw], (((1,), (1,)), ((), ())), preferred_element_type=F32
        )

    for t0, k0, kw, c0, cw in ((0, 0, 512, 0, 384), (3, 512, 512, 384, 384), (6, 1024, 256, 768, 128)):
        piece = compact(0, 512, k0, kw, c0, cw).astype(BF).reshape(2, 8, 32, cw)
        for qc in range(2):
            for t in range(cw // 128):
                gath[:, z, 7 * qc + t0 + t] = piece[qc, :, :, 128 * t:128 * t + 128]
    tail = compact(0, 256, 1024, 256, 960, 128) + compact(256, 256, 1024, 256, 896, 128)
    gath[:, z, 14] = tail.astype(BF).reshape(8, 32, 128)

    pl.semaphore_wait(barrier, 33)

    def ring(p, h, side):
        src = lax.rem(z + (8 - (h - 1)), 8) if side == 0 else lax.rem(z + (h - 1), 8)
        return pltpu.make_async_remote_copy(
            src_ref=gath.at[p, src],
            dst_ref=gath.at[p, src],
            send_sem=sent.at[1],
            recv_sem=g_recv.at[RING_SEM[side, p, h]],
            device_id=(row, zr if side == 0 else zl),
            device_id_type=MESH,
        )

    def ring_arrival(p, h, side):
        src = lax.rem(z + (8 - h), 8) if side == 0 else lax.rem(z + h, 8)
        pltpu.make_async_remote_copy(
            src_ref=gath.at[p, src],
            dst_ref=gath.at[p, src],
            send_sem=sent.at[1],
            recv_sem=g_recv.at[RING_SEM[side, p, h]],
            device_id=(row, zr if side == 0 else zl),
            device_id_type=MESH,
        ).wait_recv()

    def place_of(k):
        if k == 30:
            return row + 1 - 2 * core
        dy, dx = FAR[k // 2]
        other = core if k % 2 == 0 else 1 - core
        return (lax.rem(y + dy, 4) * 4 + lax.rem(x + dx, 4)) * 2 + other

    def peer_of(k):
        return jnp.where(core == 0, place_of(k), place_of(30 - k))

    def exchange(k):
        peer = peer_of(k)
        return pltpu.make_async_remote_copy(
            src_ref=vsend.at[pl.ds(2 * peer, 2)],
            dst_ref=vrecv.at[pl.ds(2 * row, 2)],
            send_sem=sent.at[0],
            recv_sem=a_recv.at[0],
            device_id=(peer, z),
            device_id_type=MESH,
        )

    def all_of(ref, send_sem, recv_sem):
        return pltpu.make_async_remote_copy(
            src_ref=ref, dst_ref=ref, send_sem=send_sem, recv_sem=recv_sem,
            device_id=(row, zr), device_id_type=MESH,
        )

    def build_tables():
        load_h.wait()
        load_m.wait()
        lane = lax.broadcasted_iota(jnp.int32, (40, 1280), 1)
        atom = lax.broadcasted_iota(jnp.int32, (40, 1280), 0)
        held = jnp.concatenate([jnp.broadcast_to(holder[r:r + 1, :], (40, 128)) for r in range(10)], axis=1)
        owner = lax.shift_right_logical(held * 52429, 21)
        slot = jnp.max(jnp.where(held == atom + 40 * row, lane, 0), axis=1, keepdims=True)
        source = lax.shift_right_logical(slot * 52429, 21)
        earlier = (owner == row) & (lane >= 40 * source) & (lane < slot)
        arrive = 2 * source + jnp.max(jnp.where(earlier, 1, 0), axis=1, keepdims=True)
        wanted = jnp.broadcast_to(mask[pl.ds(z, 1), :], (40, 1280))
        live = jnp.sum(jnp.where(lane == atom + 40 * row, wanted, 0), axis=1, keepdims=True)
        place = lane - 40 * row
        here = (owner == atom) & (place >= 0) & (place < 40)
        first = jnp.min(jnp.where(here, place, 39), axis=1, keepdims=True)
        last = jnp.max(jnp.where(here, place, 0), axis=1, keepdims=True)
        diagonal = lax.broadcasted_iota(jnp.int32, (40, 128), 1) == lax.broadcasted_iota(jnp.int32, (40, 128), 0)
        for r, value in enumerate((arrive, live, first, last)):
            table[r:r + 1, :] = jnp.sum(jnp.where(diagonal, value, 0), axis=0, keepdims=True)
        table[4:8, :] = jnp.zeros((4, 128), jnp.int32)
        to_scalar = pltpu.make_async_copy(table, table_s, load_sem.at[4])
        to_scalar.start()
        to_scalar.wait()

    def pack_and_send():
        build_tables()
        load_v.wait()
        for k in range(31):
            peer = peer_of(k)
            for s in range(2):
                vsend[2 * peer + s] = vin[table_s[2 + s, peer]]
            exchange(k).start()
        for s in range(2):
            vrecv[2 * row + s] = vin[table_s[2 + s, row]]

    def receive_blocks():
        all_of(vrecv.at[0:62], sent.at[0], a_recv.at[0]).wait_recv()

        def place(a, carry):
            live = jnp.full((32, 1024), table_s[1, a], jnp.int32).astype(F32).astype(BF)
            vord[pl.ds(pl.multiple_of(32 * a, 32), 32), :] = vrecv[table_s[0, a]] * live
            return carry

        lax.fori_loop(0, 40, place, 0)

    def compact_blocks():
        for k0, kw, c0, cw in ((0, 512, 0, 384), (512, 512, 384, 384), (1024, 256, 768, 128)):
            for n in range(4):
                vc[c0:c0 + cw, 256 * n:256 * n + 256] = jnp.dot(
                    smat[c0:c0 + cw, 0:kw], vord[k0:k0 + kw, 256 * n:256 * n + 256], preferred_element_type=F32
                ).astype(BF)
        vtail[...] = jnp.dot(smat[896:1088, 0:256], vord[1024:1280, :], preferred_element_type=F32).astype(BF)

    partner = row + 1 - 2 * core

    def pair_copy(p):
        return pltpu.make_async_remote_copy(
            src_ref=psend.at[p],
            dst_ref=prec.at[p],
            send_sem=sent.at[2],
            recv_sem=d_recv.at[p],
            device_id=(partner, z),
            device_id_type=MESH,
        )

    def product(p, qc, n):
        tiles = [gath[p, :, 7 * qc + t].reshape(256, 128) for t in range(7)] + [gath[p, :, 14].reshape(256, 128)]
        start = pl.multiple_of(64 * (1 - qc), 64)
        rhs = jnp.concatenate(
            [vc[:, 256 * n:256 * n + 256], vtail[pl.ds(start, 128), 256 * n:256 * n + 256]], axis=0
        )
        return jnp.dot(jnp.concatenate(tiles, axis=1), rhs, preferred_element_type=F32)

    def multiply_theirs(p):
        for n in range(4):
            psend[p, :, 256 * n:256 * n + 256] = product(p, 1 - core, n).astype(BF)
        pair_copy(p).start()

    def multiply_mine(p):
        for n in range(4):
            own[p, :, 256 * n:256 * n + 256] = product(p, core, n)

    def row_of(yy, xx):
        return (yy * 4 + xx) * 2 + core

    def first_copy(p, half, d):
        if half == 0:
            to = lax.rem(y + d, 4)
            src, dev = q.at[p, to, :, :, 0:512], row_of(to, x)
        else:
            to = lax.rem(x + d, 4)
            src, dev = q.at[p, :, to, :, 512:1024], row_of(y, to)
        return pltpu.make_async_remote_copy(
            src_ref=src,
            dst_ref=rb1.at[p, half, d - 1],
            send_sem=sent.at[3],
            recv_sem=s_recv.at[p],
            device_id=(dev, z),
            device_id_type=MESH,
        )

    def second_copy(p, half, d):
        if half == 0:
            to = lax.rem(x + d, 4)
            dev = row_of(y, to)
        else:
            to = lax.rem(y + d, 4)
            dev = row_of(to, x)
        return pltpu.make_async_remote_copy(
            src_ref=red.at[p, half, to],
            dst_ref=rb2.at[p, half, d - 1],
            send_sem=sent.at[4],
            recv_sem=t_recv.at[p],
            device_id=(dev, z),
            device_id_type=MESH,
        )

    def pair_sum(p):
        pair_copy(p).wait_recv()
        q[p] = (own[p] + prec[p].astype(F32)).astype(BF).reshape(4, 4, 16, 1024)
        for d in (2, 1, 3):
            for half in range(2):
                first_copy(p, half, d).start()

    def first_sum(p):
        all_of(rb1.at[p], sent.at[3], s_recv.at[p]).wait_recv()
        for half in range(2):
            mine = q[p, y, :, :, 0:512] if half == 0 else q[p, :, x, :, 512:1024]
            total = mine.astype(F32)
            for d in range(3):
                total = total + rb1[p, half, d].astype(F32)
            red[p, half] = total.astype(BF)
        for d in (2, 1, 3):
            for half in range(2):
                second_copy(p, half, d).start()

    def second_sum(p):
        all_of(rb2.at[p], sent.at[4], t_recv.at[p]).wait_recv()
        for half in range(2):
            total = red[p, half, x if half == 0 else y].astype(F32)
            for d in range(3):
                total = total + rb2[p, half, d].astype(F32)
            out_ref[16 * p:16 * p + 16, 512 * half:512 * half + 512] = total.astype(BF)

    packed = False
    for kind, p, h, side in build_schedule():
        if kind == "ring":
            if h > 1:
                if not packed:
                    pack_and_send()
                    packed = True
                ring_arrival(p, h - 1, side)
            ring(p, h, side).start()
        elif kind == "blocks":
            receive_blocks()
        elif kind == "compact":
            compact_blocks()
        elif kind == "theirs":
            for s in range(2):
                ring_arrival(p, hops(p)[s], s)
            multiply_theirs(p)
        elif kind == "mine":
            multiply_mine(p)
        elif kind == "pair":
            pair_sum(p)
        elif kind == "first":
            first_sum(p)
        else:
            second_sum(p)

    all_of(vsend.at[0:62], sent.at[0], a_recv.at[0]).wait_send()
    all_of(gath.at[0:7], sent.at[1], a_recv.at[0]).wait_send()
    all_of(psend, sent.at[2], a_recv.at[0]).wait_send()
    all_of(rb1, sent.at[3], a_recv.at[0]).wait_send()
    all_of(rb2, sent.at[4], a_recv.at[0]).wait_send()


def body(integrals, coeffs, mask, offsets, atom_of_slot):
    smem = pl.BlockSpec(memory_space=pltpu.SMEM)
    hbm = pl.BlockSpec(memory_space=pl.ANY)
    vmem = pltpu.VMEM
    dma = pltpu.SemaphoreType.DMA
    return pl.pallas_call(
        kernel,
        out_shape=pltpu.VMEM((128, 1024), BF),
        in_specs=[smem, hbm, hbm, hbm, hbm],
        out_specs=pl.BlockSpec(memory_space=pltpu.VMEM),
        scratch_shapes=[
            vmem((10, 128), jnp.int32),
            vmem((8, 1280), jnp.int32),
            vmem((8, 128), jnp.int32),
            pltpu.SMEM((8, 128), jnp.int32),
            vmem((40, 32, 1024), BF),
            vmem((1280, 512), BF),
            vmem((64, 32, 1024), BF),
            vmem((64, 32, 1024), BF),
            vmem((512, 1280), BF),
            vmem((1088, 512), BF),
            vmem((ROUNDS, 8, 15, 32, 128), BF),
            vmem((1280, 1024), BF),
            vmem((896, 1024), BF),
            vmem((192, 1024), BF),
            vmem((ROUNDS, 256, 1024), BF),
            vmem((ROUNDS, 256, 1024), F32),
            vmem((ROUNDS, 256, 1024), BF),
            vmem((ROUNDS, 4, 4, 16, 1024), BF),
            vmem((ROUNDS, 2, 3, 4, 16, 512), BF),
            vmem((ROUNDS, 2, 4, 16, 512), BF),
            vmem((ROUNDS, 2, 3, 16, 512), BF),
            dma((5,)),
            dma((5,)),
            dma((1,)),
            dma((len(RING_SEM),)),
            dma((ROUNDS,)),
            dma((ROUNDS,)),
            dma((ROUNDS,)),
        ],
        compiler_params=pltpu.CompilerParams(
            collective_id=0, has_side_effects=True, vmem_limit_bytes=60_000_000
        ),
    )(offsets, atom_of_slot.reshape(10, 128), mask.T, coeffs, integrals)


def solution(mesh):
    in_specs = (P("row", None, "col"), P("row", "col"), P(), P(), P())
    return jax.shard_map(body, mesh=mesh, in_specs=in_specs, out_specs=P("row", "col"), check_vma=False)
```
